32 devices in a mesh: slab: 8 (over z, x), blk: 4 (over y, core).
Axes of the slice: x: 2, y: 2, z: 4, core: 2. Of those that a mesh axis runs over, the one named last changes fastest.
Arguments:
- incident: float32 [16, 2, 336, 128], P('slab', None, 'blk'), may hold values from -6 to 6
- mie_coef: float32 [16, 2, 336], P('slab', None, 'blk'), may hold values from -0.6 to 0.6
- translation: bfloat16 [16, 8, 2, 336, 336], P('slab', None, None, 'blk'), may hold values from -0.078125 to 0.078125
- pair_shift: int32 [16, 8], P('slab'), may hold values from -1 to 1
- pair_member: int32 [16, 8], P('slab'), may hold values from 0 to 1
- positions: float32 [16, 3], P('slab'), may hold values from 0 to 1
- wave_index: int32 [256, 3], replicated, may hold values from -4 to 4
- plane_coef: bfloat16 [256, 2, 336], replicated, may hold values from -0.25 to 0.25
- ewald_weight: float32 [256], replicated, may hold values from 0.002 to 0.04
Outputs:
- basis_next: float32 [16, 2, 336, 128], P('slab', None, 'blk')
- residual: float32 [16, 2, 336, 128], P('slab', None, 'blk')
- hessenberg: float32 [9, 128], replicated
The draws below stay inside these ranges and needn't reach their ends.
Inputs may be any that keep to these rules, and one draw needn't show every extreme that they name: `pair_shift`: each pair's source sphere lies in the target's slab or in one of the two slabs beside it on the periodic cycle of slabs.
All inputs are finite; a program needn't handle non-finite values.
Results may differ from the reference program's by a relative error of at most 0.004.
Values may be sent and summed in bfloat16 or wider, within the bound.
No kernel may reach another device: no remote copies, remote signals or barrier semaphores. Data moves between devices by JAX's collectives and lax.ppermute only.
A program may use at most 64 MiB of HBM per device.

```python
import math
import jax
import jax.numpy as jnp
from jax import lax

COEF = 336
K = 8
NG = 256
SPH_DEV = 2
RHS = 128
SPHERES = 16
N_SLAB = 8


def draw_mie_coef(key, part):
    sub_one = jax.random.fold_in(key, 71)
    place = jnp.arange(SPHERES, dtype=jnp.float32) / max(SPHERES - 1, 1)
    values = jax.random.uniform(sub_one, (SPHERES, 2, COEF), jnp.float32, -0.6, 0.6)
    ramp = 0.3 + 0.7 * place
    return (values * ramp[:, None, None]).astype(jnp.float32)


def set_ends(array, rng, least, largest):
    dims = array.shape
    index_at = [jax.random.randint(jax.random.fold_in(rng, axis), (), 0, dims[axis]) for axis in range(len(dims))]
    array = array.at[tuple(index_at)].set(least)
    longest = dims.index(max(dims))
    index_at[longest] = (index_at[longest] + 1) % dims[longest]
    return array.at[tuple(index_at)].set(largest)


def block_scale(stream_key, extent, pieces, least, top_value):
    def one(position, shards_of):
        draws = jax.random.uniform(jax.random.fold_in(jax.random.fold_in(stream_key, 6), position), (shards_of,), jnp.float32, least / len(pieces), top_value / len(pieces))
        return jnp.repeat(jnp.exp(draws), extent[position] // shards_of).reshape((-1,) + (1,) * (len(extent) - position - 1))

    loudness = one(*pieces[0])
    for cut in pieces[1:]:
        loudness = loudness * one(*cut)
    return loudness


def gaussian(key, shape, scale, limit, shards=(), held_as=jnp.bfloat16):
    factor_of = block_scale(key, shape, shards, -0.22, 0.18) if shards else 1.0
    array = jax.random.normal(key, shape, jnp.float32) * scale * factor_of
    return jnp.minimum(jnp.maximum(array, -limit), limit).astype(held_as)


def setup_inputs(seed: int = 0) -> dict:
    arg_keys = jax.random.split(jax.random.key(seed), 10)
    incident = gaussian(arg_keys[0], (SPHERES, 2, COEF, RHS), 1.0, 6.0, ((0, 8), (2, 4)), jnp.float32)
    mie_coef = draw_mie_coef(jax.random.fold_in(arg_keys[9], 71), 0)
    translation = gaussian(arg_keys[2], (SPHERES, K, 2, COEF, COEF), (2 * COEF * K) ** -0.5, 0.078125, ((0, 8), (3, 4)))
    pair_shift = set_ends(jax.random.randint(arg_keys[3], (SPHERES, K), -1, 2), jax.random.fold_in(arg_keys[3], 1), -1, 1).astype(jnp.int32)
    pair_member = set_ends(jax.random.randint(arg_keys[4], (SPHERES, K), 0, SPH_DEV), jax.random.fold_in(arg_keys[4], 1), 0, SPH_DEV - 1).astype(jnp.int32)
    positions = jnp.clip(1.0 * jax.random.uniform(arg_keys[5], (SPHERES, 3), jnp.float32) ** block_scale(arg_keys[5], (SPHERES, 3), ((0, 8),), -0.2, 0.2), 0.0, 1.0)
    wave_index = set_ends(jax.random.randint(arg_keys[6], (NG, 3), -4, 5), jax.random.fold_in(arg_keys[6], 1), -4, 4).astype(jnp.int32)
    plane_coef = gaussian(arg_keys[7], (NG, 2, COEF), (2 * COEF) ** -0.5, 0.25)
    ewald_weight = jnp.clip(jnp.exp(jax.random.uniform(arg_keys[8], (NG,), jnp.float32, math.log(0.002), math.log(0.04))), 0.002, 0.04)
    return {"incident": incident, "mie_coef": mie_coef, "translation": translation, "pair_shift": pair_shift, "pair_member": pair_member, "positions": positions, "wave_index": wave_index, "plane_coef": plane_coef, "ewald_weight": ewald_weight}


two_pi = 6.283185307179586
epsilon = 1e-06
highest = lax.Precision.HIGHEST

def complex_scale(coef_pair, basis):
    part_re = coef_pair[0] * basis[:, 0] - coef_pair[1] * basis[:, 1]
    part_im = coef_pair[0] * basis[:, 1] + coef_pair[1] * basis[:, 0]
    return jnp.stack([part_re, part_im], axis=1)

def inner_sum(left, right):
    part_re = lax.optimization_barrier(jnp.sum(left[:, 0] * right[:, 0] + left[:, 1] * right[:, 1], axis=(0, 1)))
    part_im = lax.optimization_barrier(jnp.sum(left[:, 0] * right[:, 1] - left[:, 1] * right[:, 0], axis=(0, 1)))
    return jnp.stack([part_re, part_im])

def plane_sums(projected, cos_part, sin_part):
    part_re = projected[:, 0, :, 0] - projected[:, 1, :, 1]
    part_im = projected[:, 0, :, 1] + projected[:, 1, :, 0]
    sum_re = lax.optimization_barrier(jnp.sum(cos_part[:, :, None] * part_re + sin_part[:, :, None] * part_im, axis=1))
    sum_im = lax.optimization_barrier(jnp.sum(cos_part[:, :, None] * part_im - sin_part[:, :, None] * part_re, axis=1))
    return jnp.stack([sum_re, sum_im], axis=1)

def plane_field(totals, coef_full, cos_part, sin_part, weights):
    total_re = totals[:, 0][:, None, :]
    total_im = totals[:, 1][:, None, :]
    turn_re = weights[:, None, None] * (cos_part[:, :, None] * total_re - sin_part[:, :, None] * total_im)
    turn_im = weights[:, None, None] * (cos_part[:, :, None] * total_im + sin_part[:, :, None] * total_re)
    turned = jnp.stack([turn_re, turn_im], axis=1)
    projected = jnp.einsum('gac,gbjn->jabcn', coef_full, turned, precision=highest)
    return jnp.stack([projected[:, 0, 0] + projected[:, 1, 1], projected[:, 0, 1] - projected[:, 1, 0]], axis=1)

def near_field(rounded, translation, pair_shift, pair_member):

    def per_slab(slab_index):
        start_row = slab_index * SPH_DEV
        matrices = lax.dynamic_slice_in_dim(translation, start_row, SPH_DEV, 0).astype(jnp.float32)
        offsets = lax.dynamic_slice_in_dim(pair_shift, start_row, SPH_DEV, 0)
        member = lax.dynamic_slice_in_dim(pair_member, start_row, SPH_DEV, 0)
        source = (jnp.mod(slab_index + offsets, N_SLAB) * SPH_DEV + member).reshape(-1).astype(jnp.int32)
        gathered = jnp.take(rounded, source, axis=0)
        product = jnp.einsum('parc,pzcn->pazrn', matrices.reshape(SPH_DEV * K, 2, COEF, COEF), gathered, precision=highest)
        near_re = product[:, 0, 0] - product[:, 1, 1]
        near_im = product[:, 0, 1] + product[:, 1, 0]
        return jnp.stack([near_re, near_im], axis=1).reshape(SPH_DEV, K, 2, COEF, RHS).sum(axis=1)
    blocks = lax.map(per_slab, jnp.arange(N_SLAB, dtype=jnp.int32))
    return blocks.reshape(SPH_DEV * N_SLAB, 2, COEF, RHS)

def apply_operator(vector, mie_coef, translation, pair_shift, pair_member, cos_part, sin_part, coef_full, ewald_weight):
    rounded = lax.optimization_barrier(vector.astype(jnp.bfloat16)).astype(jnp.float32)
    near = near_field(rounded, translation, pair_shift, pair_member)
    projected = jnp.einsum('gac,jbcn->gajbn', coef_full, rounded, precision=highest)
    totals = plane_sums(projected, cos_part, sin_part)
    far = plane_field(totals, coef_full, cos_part, sin_part, ewald_weight)
    summed = near + far
    scaled_re = mie_coef[:, 0][:, :, None] * summed[:, 0] - mie_coef[:, 1][:, :, None] * summed[:, 1]
    scaled_im = mie_coef[:, 0][:, :, None] * summed[:, 1] + mie_coef[:, 1][:, :, None] * summed[:, 0]
    return vector - jnp.stack([scaled_re, scaled_im], axis=1)

def reference(incident, mie_coef, translation, pair_shift, pair_member, positions, wave_index, plane_coef, ewald_weight):
    entries = SPHERES * COEF
    angles = two_pi * lax.optimization_barrier(jnp.sum(wave_index.astype(jnp.float32)[:, None, :] * positions[None, :, :], axis=-1))
    cos_part = jnp.cos(angles)
    sin_part = jnp.sin(angles)
    coef_full = plane_coef.astype(jnp.float32)

    def operator(vector):
        return apply_operator(vector, mie_coef, translation, pair_shift, pair_member, cos_part, sin_part, coef_full, ewald_weight)
    beta = jnp.sqrt(lax.optimization_barrier(jnp.sum(incident * incident, axis=(0, 1, 2))) / entries + epsilon)
    first = incident / beta
    image = operator(first)
    h_one_one = inner_sum(first, image) / entries
    image = image - complex_scale(h_one_one, first)
    h_two_one = jnp.sqrt(lax.optimization_barrier(jnp.sum(image * image, axis=(0, 1, 2))) / entries + epsilon)
    basis_next = image / h_two_one
    image = operator(basis_next)
    h_one_two = inner_sum(first, image) / entries
    image = image - complex_scale(h_one_two, first)
    h_two_two = inner_sum(basis_next, image) / entries
    residual = image - complex_scale(h_two_two, basis_next)
    h_three_two = jnp.sqrt(lax.optimization_barrier(jnp.sum(residual * residual, axis=(0, 1, 2))) / entries + epsilon)
    hessenberg = jnp.stack([beta, h_one_one[0], h_one_one[1], h_two_one, h_one_two[0], h_one_two[1], h_two_two[0], h_two_two[1], h_three_two])
    return (basis_next, residual, hessenberg)
```

```python
import jax
import jax.numpy as jnp
from jax import lax
from jax.experimental import pallas as pl
from jax.experimental.pallas import tpu as pltpu
from jax.sharding import PartitionSpec as P

two_pi = 6.283185307179586
epsilon = 1e-06
f32 = jnp.float32
bf16 = jnp.bfloat16

VM = pl.BlockSpec(memory_space=pltpu.VMEM)
SM = pl.BlockSpec(memory_space=pltpu.SMEM)


def call(body, outs, specs, name):
    return pl.pallas_call(
        body,
        out_shape=outs,
        in_specs=specs,
        out_specs=jax.tree.map(lambda _: VM, outs),
        name=name,
    )


def shape(dims, dtype=f32):
    return jax.ShapeDtypeStruct(dims, dtype)


def round_body(x_ref, out_ref):
    count = out_ref.shape[2]
    for s in range(out_ref.shape[0]):
        for z in range(2):
            out_ref[s, z] = x_ref[s, pl.ds(z, count, stride=2), :].astype(bf16)


def project(field, plane_ref, cos, sin):
    sum_re = sum_im = None
    lead = (((0,), (0,)), ((), ()))
    for s in range(len(field)):
        both = jnp.concatenate(field[s], axis=1)
        with_re = lax.dot_general(plane_ref[0], both, lead, preferred_element_type=f32)
        with_im = lax.dot_general(plane_ref[1], both, lead, preferred_element_type=f32)
        n = both.shape[1] // 2
        part_re = with_re[:, :n] - with_im[:, n:]
        part_im = with_re[:, n:] + with_im[:, :n]
        c, d = cos[:, s : s + 1], sin[:, s : s + 1]
        turn_re = c * part_re + d * part_im
        turn_im = c * part_im - d * part_re
        sum_re = turn_re if sum_re is None else sum_re + turn_re
        sum_im = turn_im if sum_im is None else sum_im + turn_im
    return sum_re, sum_im


def split_halves(sum_re, sum_im, send_ref, keep_ref):
    half = sum_re.shape[0] // 2
    odd = lax.rem(lax.axis_index("blk"), 2) == 1
    n = sum_re.shape[1]
    for z, part in enumerate((sum_re, sum_im)):
        low, high = part[:half], part[half:]
        at = slice(z * n, (z + 1) * n)
        send_ref[:, at] = jnp.where(odd, low, high).astype(bf16)
        keep_ref[:, at] = jnp.where(odd, high, low)


def first_sums_body(x_ref, plane_ref, wave_ref, pos_ref, send_ref, keep_ref, cos_ref, sin_ref):
    spheres = x_ref.shape[0]
    lane = lax.broadcasted_iota(jnp.int32, (1, spheres), 1)
    turns = None
    for d in range(3):
        row = jnp.zeros((1, spheres), f32)
        for s in range(spheres):
            row = jnp.where(lane == s, pos_ref[s, d], row)
        term = wave_ref[:, d : d + 1].astype(f32) * row
        turns = term if turns is None else turns + term
    angles = two_pi * (turns - jnp.floor(turns + 0.5))
    cos, sin = jnp.cos(angles), jnp.sin(angles)
    cos_ref[...] = cos
    sin_ref[...] = sin
    field = [[x_ref[s, 0], x_ref[s, 1]] for s in range(spheres)]
    split_halves(*project(field, plane_ref, cos, sin), send_ref, keep_ref)


def gather_body(shift_ref, member_ref, *refs):
    *piece_refs, out_ref, held = refs
    blocks = len(piece_refs)
    slots, spheres, _, count, _ = piece_refs[0].shape
    b = lax.axis_index("blk")
    parity = lax.rem(lax.axis_index("slab"), 2)
    for slot in range(slots):
        for s in range(spheres):
            for z in range(2):
                parts = [ref[slot, s, z] for ref in piece_refs]
                bit = 1
                while bit < blocks:
                    swap = lax.rem(lax.div(b, bit), 2) == 1
                    parts = [
                        jnp.where(swap, parts[i ^ bit], parts[i]) for i in range(blocks)
                    ]
                    bit *= 2
                held[slot * spheres + s, z] = jnp.concatenate(parts, axis=0)
    for i in range(out_ref.shape[0]):
        for k in range(out_ref.shape[1]):
            shift = shift_ref[i, k]
            forward = (shift == 1) == (parity == 0)
            slot = jnp.where(shift == 0, 0, jnp.where(forward, 1, 2))
            out_ref[i, k] = held[slot * spheres + member_ref[i, k]]


def far_field(total, plane_ref, cos, sin, weight, spheres):
    total_re, total_im = total
    n = total_re.shape[1]
    fields = []
    for s in range(spheres):
        c, d = weight * cos[:, s : s + 1], weight * sin[:, s : s + 1]
        turned = jnp.concatenate(
            [c * total_re - d * total_im, c * total_im + d * total_re], axis=1
        ).astype(bf16)
        with_re = jnp.dot(plane_ref[0], turned, preferred_element_type=f32)
        with_im = jnp.dot(plane_ref[1], turned, preferred_element_type=f32)
        fields.append(
            (with_re[:, :n] + with_im[:, n:], with_re[:, n:] - with_im[:, :n])
        )
    return fields


def join_halves(mine_ref, other_ref):
    odd = lax.rem(lax.axis_index("blk"), 2) == 1
    n = mine_ref.shape[1] // 2
    out = []
    for z in range(2):
        at = slice(z * n, (z + 1) * n)
        mine, other = mine_ref[:, at], other_ref[:, at].astype(f32)
        out.append(
            jnp.concatenate([jnp.where(odd, other, mine), jnp.where(odd, mine, other)], axis=0)
        )
    return out


def image_fields(near_ref, mine_ref, other_ref, cos, sin, plane_ref, weight_ref, mie_ref):
    spheres = near_ref.shape[0]
    far = far_field(join_halves(mine_ref, other_ref), plane_ref, cos, sin, weight_ref[...], spheres)
    out = []
    for s in range(spheres):
        sum_re = near_ref[s, 0, 0] - near_ref[s, 1, 1] + far[s][0]
        sum_im = near_ref[s, 0, 1] + near_ref[s, 1, 0] + far[s][1]
        m_re, m_im = mie_ref[:, 2 * s : 2 * s + 1], mie_ref[:, 2 * s + 1 : 2 * s + 2]
        out.append((m_re * sum_re - m_im * sum_im, m_re * sum_im + m_im * sum_re))
    return out


def first_image_body(
    near_ref, mine_ref, other_ref, cos_ref, sin_ref, plane_ref, weight_ref, mie_ref,
    image_ref, round_ref, send_ref, keep_ref,
):
    cos, sin = cos_ref[...], sin_ref[...]
    images = image_fields(near_ref, mine_ref, other_ref, cos, sin, plane_ref, weight_ref, mie_ref)
    field = []
    for s, (re, im) in enumerate(images):
        image_ref[s, 0] = re
        image_ref[s, 1] = im
        field.append([re.astype(bf16), im.astype(bf16)])
        round_ref[s, 0] = field[s][0]
        round_ref[s, 1] = field[s][1]
    split_halves(*project(field, plane_ref, cos, sin), send_ref, keep_ref)


def second_image_body(
    near_ref, mine_ref, other_ref, cos_ref, sin_ref, plane_ref, weight_ref, mie_ref, x_ref, g_ref,
    image_ref, gram_ref,
):
    images = image_fields(
        near_ref, mine_ref, other_ref, cos_ref[...], sin_ref[...], plane_ref, weight_ref, mie_ref
    )
    count = g_ref.shape[2]
    sums = None
    for s, (re, im) in enumerate(images):
        image_ref[s, 0] = re
        image_ref[s, 1] = im
        x = (x_ref[s, pl.ds(0, count, stride=2), :], x_ref[s, pl.ds(1, count, stride=2), :])
        g = (g_ref[s, 0], g_ref[s, 1])
        h = (re, im)
        terms = [x[0] * x[0] + x[1] * x[1]]
        terms += [x[0] * g[0] + x[1] * g[1], x[0] * g[1] - x[1] * g[0]]
        terms += [g[0] * g[0] + g[1] * g[1]]
        terms += [x[0] * h[0] + x[1] * h[1], x[0] * h[1] - x[1] * h[0]]
        terms += [g[0] * h[0] + g[1] * h[1], g[0] * h[1] - g[1] * h[0]]
        terms += [h[0] * h[0] + h[1] * h[1]]
        rows = [jnp.sum(term, axis=0, keepdims=True) for term in terms]
        sums = rows if sums is None else [a + r for a, r in zip(sums, rows)]
    gram_ref[...] = jnp.zeros_like(gram_ref)
    for i, row in enumerate(sums):
        gram_ref[i : i + 1, :] = row


def times(a, b):
    return (a[0] * b[0] - a[1] * b[1], a[0] * b[1] + a[1] * b[0])


def conj_times(a, b):
    return (a[0] * b[0] + a[1] * b[1], a[0] * b[1] - a[1] * b[0])


def plus(*terms):
    return (sum(t[0] for t in terms), sum(t[1] for t in terms))


def scaled(a, r):
    return (a[0] * r, a[1] * r)


def finish_body(entries, gram_ref, x_ref, g_ref, h_ref, basis_ref, residual_ref, hess_ref):
    gram = gram_ref[...] / entries
    row = [gram[i : i + 1, :] for i in range(9)]
    xx, gg, hh = row[0], row[3], row[8]
    xg, xh, gh = (row[1], row[2]), (row[4], row[5]), (row[6], row[7])
    square = xx + epsilon
    beta = jnp.sqrt(square)
    inv = 1.0 / beta
    h11 = ((xx - xg[0]) / square, -xg[1] / square)
    alpha = ((epsilon + xg[0]) / square * inv, xg[1] / square * inv)
    delta = -inv
    cross = alpha[0] * xg[0] + alpha[1] * xg[1]
    norm = (alpha[0] * alpha[0] + alpha[1] * alpha[1]) * xx + delta * delta * gg + 2.0 * delta * cross
    h21 = jnp.sqrt(jnp.maximum(norm, 0.0) + epsilon)
    a = (alpha[0] / h21, alpha[1] / h21)
    d = delta / h21
    b = (d - a[0], -a[1])
    h12 = scaled(plus(scaled(a, xx), times(b, xg), scaled(xh, -d)), inv)
    e = (a[0] - h12[0] * inv, a[1] - h12[1] * inv)
    with_x = plus(scaled(e, xx), times(b, xg), scaled(xh, -d))
    with_g = plus(times(e, (xg[0], -xg[1])), scaled(b, gg), scaled(gh, -d))
    h22 = plus(conj_times(a, with_x), scaled(with_g, d))
    c0 = plus(e, scaled(times(h22, a), -1.0))
    c1 = plus(b, scaled(h22, -d))
    c2 = -d
    last = (
        (c0[0] * c0[0] + c0[1] * c0[1]) * xx
        + (c1[0] * c1[0] + c1[1] * c1[1]) * gg
        + c2 * c2 * hh
        + 2.0 * times(conj_times(c0, c1), xg)[0]
        + 2.0 * c2 * conj_times(c0, xh)[0]
        + 2.0 * c2 * conj_times(c1, gh)[0]
    )
    h32 = jnp.sqrt(jnp.maximum(last, 0.0) + epsilon)
    for i, value in enumerate((beta, h11[0], h11[1], h21, h12[0], h12[1], h22[0], h22[1], h32)):
        hess_ref[i : i + 1, :] = value
    count = g_ref.shape[2]
    for s in range(g_ref.shape[0]):
        rows = [pl.ds(z, count, stride=2) for z in range(2)]
        x = (x_ref[s, rows[0], :], x_ref[s, rows[1], :])
        g = (g_ref[s, 0], g_ref[s, 1])
        h = (h_ref[s, 0], h_ref[s, 1])
        basis = plus(times(a, x), scaled(g, d))
        residual = plus(times(c0, x), times(c1, g), scaled(h, c2))
        for z in range(2):
            basis_ref[s, rows[z], :] = basis[z]
            residual_ref[s, rows[z], :] = residual[z]


def trade(value, axis, bit):
    return lax.ppermute(value, axis, [(i, i ^ bit) for i in range(lax.axis_size(axis))])


def trade_odd(value):
    count = lax.axis_size("slab")
    pairs = []
    for i in range(count):
        pairs.append((i, (i + 1) % count if i % 2 else (i - 1) % count))
    return lax.ppermute(value, "slab", pairs)


def bits(axis, start=1):
    out, bit = [], start
    while bit < lax.axis_size(axis):
        out.append(bit)
        bit *= 2
    return out


def fetch_pieces(own):
    mine = jnp.stack([own, trade(own, "slab", 1), trade_odd(own)])
    pieces = {0: mine}
    for bit in bits("blk", 2):
        pieces.update({r | bit: trade(value, "blk", bit) for r, value in list(pieces.items())})
    for r, value in list(pieces.items()):
        pieces[r | 1] = trade(value, "blk", 1)
    return [pieces[r] for r in range(len(pieces))]


def total_sums(send, keep):
    keep = keep + trade(send, "blk", 1).astype(f32)
    steps = [("blk", bit) for bit in bits("blk", 2)] + [("slab", bit) for bit in bits("slab")]
    for axis, bit in steps:
        keep = keep + trade(keep.astype(bf16), axis, bit).astype(f32)
    return keep, trade(keep.astype(bf16), "blk", 1)


def total_gram(gram):
    for axis in ("blk", "slab"):
        for bit in bits(axis):
            gram = gram + trade(gram, axis, bit)
    return gram


def per_device(
    incident, mie_coef, translation, pair_shift, pair_member, positions, wave_index, plane_coef,
    ewald_weight,
):
    spheres, _, count, n = incident.shape
    pairs = translation.shape[1]
    blocks = lax.axis_size("blk")
    waves = plane_coef.shape[0]
    entries = spheres * lax.axis_size("slab") * count * blocks
    x = incident.transpose(0, 2, 1, 3).reshape(spheres, 2 * count, n)
    plane = lax.dynamic_slice_in_dim(
        plane_coef.transpose(1, 2, 0), lax.axis_index("blk") * count, count, 1
    )
    weight = ewald_weight.reshape(waves, 1)
    mie = mie_coef.transpose(2, 0, 1).reshape(count, spheres * 2)

    field = shape((spheres, 2, count, n))
    field_half = shape((spheres, 2, count, n), bf16)
    sums = shape((waves // 2, 2 * n))
    sums_half = shape((waves // 2, 2 * n), bf16)
    phase = shape((waves, spheres))
    sources = shape((spheres, pairs, 2, count * blocks, n), bf16)

    def near_products(own):
        pieces = fetch_pieces(own)
        slots = pieces[0].shape[0]
        gathered = pl.pallas_call(
            gather_body,
            out_shape=sources,
            in_specs=[SM, SM] + [VM] * blocks,
            out_specs=VM,
            scratch_shapes=[pltpu.VMEM((slots * spheres, 2, count * blocks, n), bf16)],
            name="gather",
        )(pair_shift, pair_member, *pieces)
        return jnp.einsum(
            "ikarc,ikzcn->iazrn", translation, gathered, preferred_element_type=f32
        )

    rounded = call(round_body, field_half, [VM], "round")(x)
    send, keep, cos, sin = call(
        first_sums_body, (sums_half, sums, phase, phase), [VM, VM, VM, SM], "first_sums"
    )(rounded, plane, wave_index, positions)
    mine, other = total_sums(send, keep)
    near = near_products(rounded)
    image, image_rounded, send, keep = call(
        first_image_body, (field, field_half, sums_half, sums), [VM] * 8, "first_image"
    )(near, mine, other, cos, sin, plane, weight, mie)

    mine, other = total_sums(send, keep)
    near = near_products(image_rounded)
    image_two, gram = call(second_image_body, (field, shape((16, n))), [VM] * 10, "second_image")(
        near, mine, other, cos, sin, plane, weight, mie, x, image
    )
    gram = total_gram(gram)
    flat = shape((spheres, 2 * count, n))
    basis, residual, hessenberg = call(
        lambda *refs: finish_body(float(entries), *refs), (flat, flat, shape((9, n))), [VM] * 4, "finish"
    )(gram, x, image, image_two)

    def unflatten(value):
        return value.reshape(spheres, count, 2, n).transpose(0, 2, 1, 3)

    return unflatten(basis), unflatten(residual), hessenberg


def solution(mesh):
    placed = (
        P("slab", None, "blk", None),
        P("slab", None, "blk"),
        P("slab", None, None, "blk", None),
        P("slab", None),
        P("slab", None),
        P("slab", None),
        P(),
        P(),
        P(),
    )
    return jax.shard_map(
        per_device,
        mesh=mesh,
        in_specs=placed,
        out_specs=(P("slab", None, "blk", None), P("slab", None, "blk", None), P()),
        check_vma=False,
    )
```

```python
import jax
import jax.numpy as jnp
from jax import lax
from jax.experimental import pallas as pl
from jax.experimental.pallas import tpu as pltpu
from jax.sharding import PartitionSpec as P

two_pi = 6.283185307179586
epsilon = 1e-06
f32 = jnp.float32
bf16 = jnp.bfloat16

VM = pl.BlockSpec(memory_space=pltpu.VMEM)
SM = pl.BlockSpec(memory_space=pltpu.SMEM)


def call(body, outs, specs, name, scratch=()):
    return pl.pallas_call(
        body,
        out_shape=outs,
        in_specs=specs,
        out_specs=jax.tree.map(lambda _: VM, outs),
        scratch_shapes=scratch,
        compiler_params=pltpu.CompilerParams(vmem_limit_bytes=16 << 20),
        name=name,
    )


def shape(dims, dtype=f32):
    return jax.ShapeDtypeStruct(dims, dtype)


def round_body(x_ref, out_ref):
    count = out_ref.shape[2]
    for s in range(out_ref.shape[0]):
        for z in range(2):
            out_ref[s, z] = x_ref[s, pl.ds(z, count, stride=2), :].astype(bf16)


def project(field, plane_ref, columns, spheres):
    sum_re = sum_im = None
    lead = (((0,), (0,)), ((), ()))
    for s in range(len(field)):
        both = jnp.concatenate(field[s], axis=1)
        with_re = lax.dot_general(plane_ref[0], both, lead, preferred_element_type=f32)
        with_im = lax.dot_general(plane_ref[1], both, lead, preferred_element_type=f32)
        n = both.shape[1] // 2
        part_re = with_re[:, :n] - with_im[:, n:]
        part_im = with_re[:, n:] + with_im[:, :n]
        c, d = columns[:, s : s + 1], columns[:, spheres + s : spheres + s + 1]
        turn_re = c * part_re + d * part_im
        turn_im = c * part_im - d * part_re
        sum_re = turn_re if sum_re is None else sum_re + turn_re
        sum_im = turn_im if sum_im is None else sum_im + turn_im
    return sum_re, sum_im


def split_halves(sum_re, sum_im, send_ref, keep_ref):
    half = sum_re.shape[0] // 2
    odd = lax.rem(lax.axis_index("blk"), 2) == 1
    n = sum_re.shape[1]
    for z, part in enumerate((sum_re, sum_im)):
        low, high = part[:half], part[half:]
        at = slice(z * n, (z + 1) * n)
        send_ref[:, at] = jnp.where(odd, low, high).astype(bf16)
        keep_ref[:, at] = jnp.where(odd, high, low)


def first_sums_body(
    x_ref, plane_ref, wave_ref, pos_ref, weight_ref, mie_ref,
    send_ref, keep_ref, column_ref, part_ref, held,
):
    spheres, _, count, _ = x_ref.shape
    waves = wave_ref.shape[1]
    b = lax.axis_index("blk")
    for a in range(2):
        part = plane_ref[a, 0:count, :]
        for p in range(1, plane_ref.shape[1] // count):
            part = jnp.where(b == p, plane_ref[a, p * count : (p + 1) * count, :], part)
        part_ref[a] = part
    row = lax.broadcasted_iota(jnp.int32, (spheres, 1), 0)
    turns = None
    for d in range(3):
        place = jnp.zeros((spheres, 1), f32)
        for s in range(spheres):
            place = jnp.where(row == s, pos_ref[s, d], place)
        term = wave_ref[d : d + 1, :].astype(f32) * place
        turns = term if turns is None else turns + term
    angles = two_pi * (turns - jnp.floor(turns + 0.5))
    cos, sin = jnp.cos(angles), jnp.sin(angles)
    weight = weight_ref[...]
    held[...] = jnp.zeros_like(held)
    for i, value in enumerate((cos, sin, weight * cos, weight * sin)):
        held[i * spheres : (i + 1) * spheres, :] = value
    for s in range(spheres):
        for z in range(2):
            at = 4 * spheres + 2 * s + z
            held[at : at + 1, 0:count] = mie_ref[s, z : z + 1, :]
    columns = held[...].T
    column_ref[...] = columns
    field = [[x_ref[s, 0], x_ref[s, 1]] for s in range(spheres)]
    split_halves(*project(field, part_ref, columns, spheres), send_ref, keep_ref)


def gather_body(shift_ref, member_ref, *refs):
    *piece_refs, out_ref, held = refs
    blocks = len(piece_refs)
    slots, spheres, _, count, _ = piece_refs[0].shape
    b = lax.axis_index("blk")
    parity = lax.rem(lax.axis_index("slab"), 2)
    for slot in range(slots):
        for s in range(spheres):
            for z in range(2):
                parts = [ref[slot, s, z] for ref in piece_refs]
                bit = 1
                while bit < blocks:
                    swap = lax.rem(lax.div(b, bit), 2) == 1
                    parts = [
                        jnp.where(swap, parts[i ^ bit], parts[i]) for i in range(blocks)
                    ]
                    bit *= 2
                held[slot * spheres + s, z] = jnp.concatenate(parts, axis=0)
    for i in range(out_ref.shape[0]):
        for k in range(out_ref.shape[1]):
            shift = shift_ref[i, k]
            forward = (shift == 1) == (parity == 0)
            slot = jnp.where(shift == 0, 0, jnp.where(forward, 1, 2))
            out_ref[i, k] = held[slot * spheres + member_ref[i, k]]


def far_field(total, plane_ref, columns, spheres):
    total_re, total_im = total
    n = total_re.shape[1]
    fields = []
    for s in range(spheres):
        at = 2 * spheres + s
        c, d = columns[:, at : at + 1], columns[:, at + spheres : at + spheres + 1]
        turned = jnp.concatenate(
            [c * total_re - d * total_im, c * total_im + d * total_re], axis=1
        ).astype(bf16)
        with_re = jnp.dot(plane_ref[0], turned, preferred_element_type=f32)
        with_im = jnp.dot(plane_ref[1], turned, preferred_element_type=f32)
        fields.append(
            (with_re[:, :n] + with_im[:, n:], with_re[:, n:] - with_im[:, :n])
        )
    return fields


def join_halves(mine_ref, other_ref):
    odd = lax.rem(lax.axis_index("blk"), 2) == 1
    n = mine_ref.shape[1] // 2
    out = []
    for z in range(2):
        at = slice(z * n, (z + 1) * n)
        mine, other = mine_ref[:, at], other_ref[:, at].astype(f32)
        out.append(
            jnp.concatenate([jnp.where(odd, other, mine), jnp.where(odd, mine, other)], axis=0)
        )
    return out


def image_fields(near_ref, mine_ref, other_ref, column_ref, plane_ref):
    spheres, pairs, _, _, count, _ = near_ref.shape
    far = far_field(join_halves(mine_ref, other_ref), plane_ref, column_ref[...], spheres)
    out = []
    for s in range(spheres):
        sum_re, sum_im = far[s]
        for k in range(pairs):
            sum_re = sum_re + (near_ref[s, k, 0, 0] - near_ref[s, k, 1, 1])
            sum_im = sum_im + (near_ref[s, k, 0, 1] + near_ref[s, k, 1, 0])
        at = 4 * spheres + 2 * s
        m_re = column_ref[0:count, at : at + 1]
        m_im = column_ref[0:count, at + 1 : at + 2]
        out.append((m_re * sum_re - m_im * sum_im, m_re * sum_im + m_im * sum_re))
    return out


def first_image_body(
    near_ref, mine_ref, other_ref, column_ref, plane_ref,
    image_ref, round_ref, send_ref, keep_ref,
):
    images = image_fields(near_ref, mine_ref, other_ref, column_ref, plane_ref)
    field = []
    for s, (re, im) in enumerate(images):
        image_ref[s, 0] = re
        image_ref[s, 1] = im
        field.append([re.astype(bf16), im.astype(bf16)])
        round_ref[s, 0] = field[s][0]
        round_ref[s, 1] = field[s][1]
    sums = project(field, plane_ref, column_ref[...], len(images))
    split_halves(*sums, send_ref, keep_ref)


def second_image_body(
    near_ref, mine_ref, other_ref, column_ref, plane_ref, x_ref, g_ref, image_ref, gram_ref,
):
    images = image_fields(near_ref, mine_ref, other_ref, column_ref, plane_ref)
    count = g_ref.shape[2]
    sums = None
    for s, (re, im) in enumerate(images):
        image_ref[s, 0] = re
        image_ref[s, 1] = im
        x = (x_ref[s, pl.ds(0, count, stride=2), :], x_ref[s, pl.ds(1, count, stride=2), :])
        g = (g_ref[s, 0], g_ref[s, 1])
        h = (re, im)
        terms = [x[0] * x[0] + x[1] * x[1]]
        terms += [x[0] * g[0] + x[1] * g[1], x[0] * g[1] - x[1] * g[0]]
        terms += [g[0] * g[0] + g[1] * g[1]]
        terms += [x[0] * h[0] + x[1] * h[1], x[0] * h[1] - x[1] * h[0]]
        terms += [g[0] * h[0] + g[1] * h[1], g[0] * h[1] - g[1] * h[0]]
        terms += [h[0] * h[0] + h[1] * h[1]]
        rows = [jnp.sum(term, axis=0, keepdims=True) for term in terms]
        sums = rows if sums is None else [a + r for a, r in zip(sums, rows)]
    gram_ref[...] = jnp.zeros_like(gram_ref)
    for i, row in enumerate(sums):
        gram_ref[i : i + 1, :] = row


def times(a, b):
    return (a[0] * b[0] - a[1] * b[1], a[0] * b[1] + a[1] * b[0])


def conj_times(a, b):
    return (a[0] * b[0] + a[1] * b[1], a[0] * b[1] - a[1] * b[0])


def plus(*terms):
    return (sum(t[0] for t in terms), sum(t[1] for t in terms))


def scaled(a, r):
    return (a[0] * r, a[1] * r)


def finish_body(entries, gram_ref, x_ref, g_ref, h_ref, basis_ref, residual_ref, hess_ref):
    gram = gram_ref[...] / entries
    row = [gram[i : i + 1, :] for i in range(9)]
    xx, gg, hh = row[0], row[3], row[8]
    xg, xh, gh = (row[1], row[2]), (row[4], row[5]), (row[6], row[7])
    square = xx + epsilon
    beta = jnp.sqrt(square)
    inv = 1.0 / beta
    h11 = ((xx - xg[0]) / square, -xg[1] / square)
    alpha = ((epsilon + xg[0]) / square * inv, xg[1] / square * inv)
    delta = -inv
    cross = alpha[0] * xg[0] + alpha[1] * xg[1]
    norm = (alpha[0] * alpha[0] + alpha[1] * alpha[1]) * xx + delta * delta * gg + 2.0 * delta * cross
    h21 = jnp.sqrt(jnp.maximum(norm, 0.0) + epsilon)
    a = (alpha[0] / h21, alpha[1] / h21)
    d = delta / h21
    b = (d - a[0], -a[1])
    h12 = scaled(plus(scaled(a, xx), times(b, xg), scaled(xh, -d)), inv)
    e = (a[0] - h12[0] * inv, a[1] - h12[1] * inv)
    with_x = plus(scaled(e, xx), times(b, xg), scaled(xh, -d))
    with_g = plus(times(e, (xg[0], -xg[1])), scaled(b, gg), scaled(gh, -d))
    h22 = plus(conj_times(a, with_x), scaled(with_g, d))
    c0 = plus(e, scaled(times(h22, a), -1.0))
    c1 = plus(b, scaled(h22, -d))
    c2 = -d
    last = (
        (c0[0] * c0[0] + c0[1] * c0[1]) * xx
        + (c1[0] * c1[0] + c1[1] * c1[1]) * gg
        + c2 * c2 * hh
        + 2.0 * times(conj_times(c0, c1), xg)[0]
        + 2.0 * c2 * conj_times(c0, xh)[0]
        + 2.0 * c2 * conj_times(c1, gh)[0]
    )
    h32 = jnp.sqrt(jnp.maximum(last, 0.0) + epsilon)
    for i, value in enumerate((beta, h11[0], h11[1], h21, h12[0], h12[1], h22[0], h22[1], h32)):
        hess_ref[i : i + 1, :] = value
    count = g_ref.shape[2]
    for s in range(g_ref.shape[0]):
        rows = [pl.ds(z, count, stride=2) for z in range(2)]
        x = (x_ref[s, rows[0], :], x_ref[s, rows[1], :])
        g = (g_ref[s, 0], g_ref[s, 1])
        h = (h_ref[s, 0], h_ref[s, 1])
        basis = plus(times(a, x), scaled(g, d))
        residual = plus(times(c0, x), times(c1, g), scaled(h, c2))
        for z in range(2):
            basis_ref[s, rows[z], :] = basis[z]
            residual_ref[s, rows[z], :] = residual[z]


def trade(value, axis, bit):
    return lax.ppermute(value, axis, [(i, i ^ bit) for i in range(lax.axis_size(axis))])


def trade_odd(value):
    count = lax.axis_size("slab")
    pairs = []
    for i in range(count):
        pairs.append((i, (i + 1) % count if i % 2 else (i - 1) % count))
    return lax.ppermute(value, "slab", pairs)


def bits(axis, start=1):
    out, bit = [], start
    while bit < lax.axis_size(axis):
        out.append(bit)
        bit *= 2
    return out


def fetch_pieces(own):
    mine = jnp.stack([own, trade(own, "slab", 1), trade_odd(own)])
    pieces = {0: mine}
    for bit in bits("blk", 2):
        pieces.update({r | bit: trade(value, "blk", bit) for r, value in list(pieces.items())})
    for r, value in list(pieces.items()):
        pieces[r | 1] = trade(value, "blk", 1)
    return [pieces[r] for r in range(len(pieces))]


def total_sums(send, keep):
    keep = keep + trade(send, "blk", 1).astype(f32)
    steps = [("blk", bit) for bit in bits("blk", 2)] + [("slab", bit) for bit in bits("slab")]
    for axis, bit in steps:
        keep = keep + trade(keep.astype(bf16), axis, bit).astype(f32)
    return keep, trade(keep.astype(bf16), "blk", 1)


def total_gram(gram):
    for axis in ("blk", "slab"):
        for bit in bits(axis):
            gram = gram + trade(gram, axis, bit)
    return gram


def per_device(
    incident, mie_coef, translation, pair_shift, pair_member, positions, wave_index, plane_coef,
    ewald_weight,
):
    spheres, _, count, n = incident.shape
    pairs = translation.shape[1]
    blocks = lax.axis_size("blk")
    waves = plane_coef.shape[0]
    entries = spheres * lax.axis_size("slab") * count * blocks
    x = incident.transpose(0, 2, 1, 3).reshape(spheres, 2 * count, n)
    plane = plane_coef.transpose(1, 2, 0)

    field = shape((spheres, 2, count, n))
    field_half = shape((spheres, 2, count, n), bf16)
    sums = shape((waves // 2, 2 * n))
    sums_half = shape((waves // 2, 2 * n), bf16)
    sources = shape((spheres, pairs, 2, count * blocks, n), bf16)
    held_rows = -(-6 * spheres // 8) * 8
    column = shape((waves, held_rows))
    part = shape((2, count, waves), bf16)

    def near_products(own):
        pieces = fetch_pieces(own)
        slots = pieces[0].shape[0]
        held = pltpu.VMEM((slots * spheres, 2, count * blocks, n), bf16)
        gathered = call(gather_body, sources, [SM, SM] + [VM] * blocks, "gather", [held])(
            pair_shift, pair_member, *pieces
        )
        return jnp.einsum(
            "ikarc,ikzcn->ikazrn", translation, gathered, preferred_element_type=f32
        )

    rounded = call(round_body, field_half, [VM], "round")(x)
    send, keep, columns, plane = call(
        first_sums_body,
        (sums_half, sums, column, part),
        [VM, VM, VM, SM, VM, VM],
        "first_sums",
        [pltpu.VMEM((held_rows, waves), f32)],
    )(rounded, plane, wave_index.T, positions, ewald_weight.reshape(1, waves), mie_coef)
    mine, other = total_sums(send, keep)
    near = near_products(rounded)
    image, image_rounded, send, keep = call(
        first_image_body, (field, field_half, sums_half, sums), [VM] * 5, "first_image"
    )(near, mine, other, columns, plane)

    mine, other = total_sums(send, keep)
    near = near_products(image_rounded)
    image_two, gram = call(second_image_body, (field, shape((16, n))), [VM] * 7, "second_image")(
        near, mine, other, columns, plane, x, image
    )
    gram = total_gram(gram)
    flat = shape((spheres, 2 * count, n))
    basis, residual, hessenberg = call(
        lambda *refs: finish_body(float(entries), *refs), (flat, flat, shape((9, n))), [VM] * 4, "finish"
    )(gram, x, image, image_two)

    def unflatten(value):
        return value.reshape(spheres, count, 2, n).transpose(0, 2, 1, 3)

    return unflatten(basis), unflatten(residual), hessenberg


def solution(mesh):
    placed = (
        P("slab", None, "blk", None),
        P("slab", None, "blk"),
        P("slab", None, None, "blk", None),
        P("slab", None),
        P("slab", None),
        P("slab", None),
        P(),
        P(),
        P(),
    )
    return jax.shard_map(
        per_device,
        mesh=mesh,
        in_specs=placed,
        out_specs=(P("slab", None, "blk", None), P("slab", None, "blk", None), P()),
        check_vma=False,
    )
```

```python
import jax
import jax.numpy as jnp
from jax import lax
from jax.experimental import pallas as pl
from jax.experimental.pallas import tpu as pltpu
from jax.sharding import PartitionSpec as P

two_pi = 6.283185307179586
epsilon = 1e-06
f32 = jnp.float32
bf16 = jnp.bfloat16

VM = pl.BlockSpec(memory_space=pltpu.VMEM)
SM = pl.BlockSpec(memory_space=pltpu.SMEM)
HB = pl.BlockSpec(memory_space=pltpu.HBM)


def call(body, outs, specs, scratch=()):
    return pl.pallas_call(
        body,
        out_shape=outs,
        in_specs=specs,
        out_specs=jax.tree.map(lambda _: VM, outs),
        scratch_shapes=scratch,
        compiler_params=pltpu.CompilerParams(vmem_limit_bytes=16 << 20),
    )


def in_hbm(arrays):
    return [pltpu.with_memory_space_constraint(v, pltpu.HBM) for v in arrays]


def shape(dims, dtype=f32):
    return jax.ShapeDtypeStruct(dims, dtype)


def project(field, plane_ref, columns, spheres):
    sum_re = sum_im = None
    lead = (((0,), (0,)), ((), ()))
    for s in range(len(field)):
        both = jnp.concatenate(field[s], axis=1)
        with_re = lax.dot_general(plane_ref[0], both, lead, preferred_element_type=f32)
        with_im = lax.dot_general(plane_ref[1], both, lead, preferred_element_type=f32)
        n = both.shape[1] // 2
        part_re = with_re[:, :n] - with_im[:, n:]
        part_im = with_re[:, n:] + with_im[:, :n]
        c, d = columns[:, s : s + 1], columns[:, spheres + s : spheres + s + 1]
        turn_re = c * part_re + d * part_im
        turn_im = c * part_im - d * part_re
        sum_re = turn_re if sum_re is None else sum_re + turn_re
        sum_im = turn_im if sum_im is None else sum_im + turn_im
    return sum_re, sum_im


def split_halves(sum_re, sum_im, send_ref, keep_ref):
    half = sum_re.shape[0] // 2
    odd = lax.rem(lax.axis_index("blk"), 2) == 1
    n = sum_re.shape[1]
    for z, part in enumerate((sum_re, sum_im)):
        low, high = part[:half], part[half:]
        at = slice(z * n, (z + 1) * n)
        send_ref[:, at] = jnp.where(odd, low, high).astype(bf16)
        keep_ref[:, at] = jnp.where(odd, high, low)


def first_sums_body(
    x_hbm, plane_hbm, wave_hbm, pos_hbm, weight_hbm, mie_hbm,
    round_ref, send_ref, keep_ref, column_ref, part_ref,
    x_ref, plane_ref, wave_ref, pos_ref, weight_ref, mie_ref, held, sems,
):
    moves = ((wave_hbm, wave_ref), (pos_hbm, pos_ref), (weight_hbm, weight_ref), (mie_hbm, mie_ref))
    moves += ((plane_hbm, plane_ref), (x_hbm, x_ref))
    copies = [pltpu.make_async_copy(*move, sems.at[i]) for i, move in enumerate(moves)]
    for copy in copies:
        copy.start()
    for copy in copies:
        copy.wait()
    spheres, _, count, _ = round_ref.shape
    b = lax.axis_index("blk")
    for a in range(2):
        part = plane_ref[a, 0:count, :]
        for p in range(1, plane_ref.shape[1] // count):
            part = jnp.where(b == p, plane_ref[a, p * count : (p + 1) * count, :], part)
        part_ref[a] = part
    turns = None
    for d in range(3):
        term = wave_ref[d : d + 1, :].astype(f32) * pos_ref[:, d : d + 1]
        turns = term if turns is None else turns + term
    angles = two_pi * (turns - jnp.floor(turns + 0.5))
    cos, sin = jnp.cos(angles), jnp.sin(angles)
    weight = weight_ref[...]
    held[...] = jnp.zeros_like(held)
    for i, value in enumerate((cos, sin, weight * cos, weight * sin)):
        held[i * spheres : (i + 1) * spheres, :] = value
    for s in range(spheres):
        for z in range(2):
            at = 4 * spheres + 2 * s + z
            held[at : at + 1, 0:count] = mie_ref[s, z : z + 1, :]
    columns = held[...].T
    column_ref[...] = columns
    field = []
    for s in range(spheres):
        field.append([x_ref[s, pl.ds(z, count, stride=2), :].astype(bf16) for z in range(2)])
        round_ref[s, 0] = field[s][0]
        round_ref[s, 1] = field[s][1]
    split_halves(*project(field, part_ref, columns, spheres), send_ref, keep_ref)


def gather_body(shift_hbm, member_hbm, *refs):
    *piece_refs, out_ref, held, shift_ref, member_ref, sems = refs
    copies = [
        pltpu.make_async_copy(shift_hbm, shift_ref, sems.at[0]),
        pltpu.make_async_copy(member_hbm, member_ref, sems.at[1]),
    ]
    for copy in copies:
        copy.start()
    blocks = len(piece_refs) // 2
    near_refs, odd_refs = piece_refs[:blocks], piece_refs[blocks:]
    spheres, _, _, _ = odd_refs[0].shape
    b = lax.axis_index("blk")
    parity = lax.rem(lax.axis_index("slab"), 2)
    for slot in range(3):
        for s in range(spheres):
            for z in range(2):
                if slot < 2:
                    parts = [ref[slot, s, z] for ref in near_refs]
                else:
                    parts = [ref[s, z] for ref in odd_refs]
                bit = 1
                while bit < blocks:
                    swap = lax.rem(lax.div(b, bit), 2) == 1
                    parts = [
                        jnp.where(swap, parts[i ^ bit], parts[i]) for i in range(blocks)
                    ]
                    bit *= 2
                held[slot * spheres + s, z] = jnp.concatenate(parts, axis=0)
    for copy in copies:
        copy.wait()
    for i in range(out_ref.shape[0]):
        for k in range(out_ref.shape[1]):
            shift = shift_ref[i, k]
            forward = (shift == 1) == (parity == 0)
            slot = jnp.where(shift == 0, 0, jnp.where(forward, 1, 2))
            out_ref[i, k] = held[slot * spheres + member_ref[i, k]]


def far_field(total, plane_ref, columns, spheres):
    total_re, total_im = total
    n = total_re.shape[1]
    fields = []
    for s in range(spheres):
        at = 2 * spheres + s
        c, d = columns[:, at : at + 1], columns[:, at + spheres : at + spheres + 1]
        turned = jnp.concatenate(
            [c * total_re - d * total_im, c * total_im + d * total_re], axis=1
        ).astype(bf16)
        with_re = jnp.dot(plane_ref[0], turned, preferred_element_type=f32)
        with_im = jnp.dot(plane_ref[1], turned, preferred_element_type=f32)
        fields.append(
            (with_re[:, :n] + with_im[:, n:], with_re[:, n:] - with_im[:, :n])
        )
    return fields


def join_halves(mine_ref, other_ref):
    odd = lax.rem(lax.axis_index("blk"), 2) == 1
    n = mine_ref.shape[1] // 2
    out = []
    for z in range(2):
        at = slice(z * n, (z + 1) * n)
        mine, other = mine_ref[:, at], other_ref[:, at].astype(f32)
        out.append(
            jnp.concatenate([jnp.where(odd, other, mine), jnp.where(odd, mine, other)], axis=0)
        )
    return out


def image_fields(near_ref, mine_ref, other_ref, column_ref, plane_ref):
    spheres, pairs, _, _, count, _ = near_ref.shape
    far = far_field(join_halves(mine_ref, other_ref), plane_ref, column_ref[...], spheres)
    out = []
    for s in range(spheres):
        sum_re, sum_im = far[s]
        for k in range(pairs):
            sum_re = sum_re + (near_ref[s, k, 0, 0] - near_ref[s, k, 1, 1])
            sum_im = sum_im + (near_ref[s, k, 0, 1] + near_ref[s, k, 1, 0])
        at = 4 * spheres + 2 * s
        m_re = column_ref[0:count, at : at + 1]
        m_im = column_ref[0:count, at + 1 : at + 2]
        out.append((m_re * sum_re - m_im * sum_im, m_re * sum_im + m_im * sum_re))
    return out


def first_image_body(
    near_ref, mine_ref, other_ref, column_ref, plane_ref,
    image_ref, round_ref, send_ref, keep_ref,
):
    images = image_fields(near_ref, mine_ref, other_ref, column_ref, plane_ref)
    field = []
    for s, (re, im) in enumerate(images):
        image_ref[s, 0] = re
        image_ref[s, 1] = im
        field.append([re.astype(bf16), im.astype(bf16)])
        round_ref[s, 0] = field[s][0]
        round_ref[s, 1] = field[s][1]
    sums = project(field, plane_ref, column_ref[...], len(images))
    split_halves(*sums, send_ref, keep_ref)


def second_image_body(
    near_ref, mine_ref, other_ref, column_ref, plane_ref, x_ref, g_ref, image_ref, gram_ref,
):
    images = image_fields(near_ref, mine_ref, other_ref, column_ref, plane_ref)
    count = g_ref.shape[2]
    sums = None
    for s, (re, im) in enumerate(images):
        image_ref[s, 0] = re
        image_ref[s, 1] = im
        x = (x_ref[s, pl.ds(0, count, stride=2), :], x_ref[s, pl.ds(1, count, stride=2), :])
        g = (g_ref[s, 0], g_ref[s, 1])
        h = (re, im)
        terms = [x[0] * x[0] + x[1] * x[1]]
        terms += [x[0] * g[0] + x[1] * g[1], x[0] * g[1] - x[1] * g[0]]
        terms += [g[0] * g[0] + g[1] * g[1]]
        terms += [x[0] * h[0] + x[1] * h[1], x[0] * h[1] - x[1] * h[0]]
        terms += [g[0] * h[0] + g[1] * h[1], g[0] * h[1] - g[1] * h[0]]
        terms += [h[0] * h[0] + h[1] * h[1]]
        rows = [jnp.sum(term, axis=0, keepdims=True) for term in terms]
        sums = rows if sums is None else [a + r for a, r in zip(sums, rows)]
    gram_ref[...] = jnp.zeros_like(gram_ref)
    for i, row in enumerate(sums):
        gram_ref[i : i + 1, :] = row


def times(a, b):
    return (a[0] * b[0] - a[1] * b[1], a[0] * b[1] + a[1] * b[0])


def conj_times(a, b):
    return (a[0] * b[0] + a[1] * b[1], a[0] * b[1] - a[1] * b[0])


def plus(*terms):
    return (sum(t[0] for t in terms), sum(t[1] for t in terms))


def scaled(a, r):
    return (a[0] * r, a[1] * r)


def finish_body(entries, gram_ref, x_ref, g_ref, h_ref, basis_ref, residual_ref, hess_ref):
    gram = gram_ref[...] / entries
    row = [gram[i : i + 1, :] for i in range(9)]
    xx, gg, hh = row[0], row[3], row[8]
    xg, xh, gh = (row[1], row[2]), (row[4], row[5]), (row[6], row[7])
    square = xx + epsilon
    beta = jnp.sqrt(square)
    inv = 1.0 / beta
    h11 = ((xx - xg[0]) / square, -xg[1] / square)
    alpha = ((epsilon + xg[0]) / square * inv, xg[1] / square * inv)
    delta = -inv
    cross = alpha[0] * xg[0] + alpha[1] * xg[1]
    norm = (alpha[0] * alpha[0] + alpha[1] * alpha[1]) * xx + delta * delta * gg + 2.0 * delta * cross
    h21 = jnp.sqrt(jnp.maximum(norm, 0.0) + epsilon)
    a = (alpha[0] / h21, alpha[1] / h21)
    d = delta / h21
    b = (d - a[0], -a[1])
    h12 = scaled(plus(scaled(a, xx), times(b, xg), scaled(xh, -d)), inv)
    e = (a[0] - h12[0] * inv, a[1] - h12[1] * inv)
    with_x = plus(scaled(e, xx), times(b, xg), scaled(xh, -d))
    with_g = plus(times(e, (xg[0], -xg[1])), scaled(b, gg), scaled(gh, -d))
    h22 = plus(conj_times(a, with_x), scaled(with_g, d))
    c0 = plus(e, scaled(times(h22, a), -1.0))
    c1 = plus(b, scaled(h22, -d))
    c2 = -d
    last = (
        (c0[0] * c0[0] + c0[1] * c0[1]) * xx
        + (c1[0] * c1[0] + c1[1] * c1[1]) * gg
        + c2 * c2 * hh
        + 2.0 * times(conj_times(c0, c1), xg)[0]
        + 2.0 * c2 * conj_times(c0, xh)[0]
        + 2.0 * c2 * conj_times(c1, gh)[0]
    )
    h32 = jnp.sqrt(jnp.maximum(last, 0.0) + epsilon)
    for i, value in enumerate((beta, h11[0], h11[1], h21, h12[0], h12[1], h22[0], h22[1], h32)):
        hess_ref[i : i + 1, :] = value
    count = g_ref.shape[2]
    for s in range(g_ref.shape[0]):
        rows = [pl.ds(z, count, stride=2) for z in range(2)]
        x = (x_ref[s, rows[0], :], x_ref[s, rows[1], :])
        g = (g_ref[s, 0], g_ref[s, 1])
        h = (h_ref[s, 0], h_ref[s, 1])
        basis = plus(times(a, x), scaled(g, d))
        residual = plus(times(c0, x), times(c1, g), scaled(h, c2))
        for z in range(2):
            basis_ref[s, rows[z], :] = basis[z]
            residual_ref[s, rows[z], :] = residual[z]


def trade(value, axis, bit):
    return lax.ppermute(value, axis, [(i, i ^ bit) for i in range(lax.axis_size(axis))])


def trade_odd(value):
    count = lax.axis_size("slab")
    pairs = []
    for i in range(count):
        pairs.append((i, (i + 1) % count if i % 2 else (i - 1) % count))
    return lax.ppermute(value, "slab", pairs)


def trade_mixed(value, even, odd):
    blocks = lax.axis_size("blk")
    pairs = []
    for i in range(blocks * lax.axis_size("slab")):
        axis, bit = odd if i % 2 else even
        pairs.append((i, i ^ (bit if axis == "blk" else bit * blocks)))
    return lax.ppermute(value, ("slab", "blk"), pairs)


def bits(axis, start=1):
    out, bit = [], start
    while bit < lax.axis_size(axis):
        out.append(bit)
        bit *= 2
    return out


def fetch_pieces(own):
    out = []
    even = trade(own, "slab", 1)
    groups = [jnp.stack([own, even]), trade_odd(own)]
    for group in groups:
        pieces = {0: group}
        for bit in bits("blk", 2):
            pieces.update({r | bit: trade(value, "blk", bit) for r, value in list(pieces.items())})
        for r, value in list(pieces.items()):
            pieces[r | 1] = trade(value, "blk", 1)
        out += [pieces[r] for r in range(len(pieces))]
    return out


def total_sums(send, keep):
    keep = keep + trade(send, "blk", 1).astype(f32)
    steps = [("blk", bit) for bit in bits("blk", 2)] + [("slab", bit) for bit in bits("slab")]
    crossed = steps[1::-1] + steps[2:] if len(steps) > 1 else steps
    for even, odd in zip(steps, crossed):
        keep = keep + trade_mixed(keep.astype(bf16), even, odd).astype(f32)
    return keep, trade(keep.astype(bf16), "blk", 1)


def total_gram(gram):
    for axis in ("blk", "slab"):
        for bit in bits(axis):
            gram = gram + trade(gram, axis, bit)
    return gram


def per_device(
    incident, mie_coef, translation, pair_shift, pair_member, positions, wave_index, plane_coef,
    ewald_weight,
):
    spheres, _, count, n = incident.shape
    pairs = translation.shape[1]
    blocks = lax.axis_size("blk")
    waves = plane_coef.shape[0]
    entries = spheres * lax.axis_size("slab") * count * blocks
    x = incident.transpose(0, 2, 1, 3).reshape(spheres, 2 * count, n)
    plane = plane_coef.transpose(1, 2, 0)

    field = shape((spheres, 2, count, n))
    field_half = shape((spheres, 2, count, n), bf16)
    sums = shape((waves // 2, 2 * n))
    sums_half = shape((waves // 2, 2 * n), bf16)
    sources = shape((spheres, pairs, 2, count * blocks, n), bf16)
    held_rows = -(-6 * spheres // 8) * 8
    column = shape((waves, held_rows))
    part = shape((2, count, waves), bf16)

    def near_products(own):
        pieces = fetch_pieces(own)
        table = pltpu.SMEM((spheres, pairs), jnp.int32)
        buffers = [pltpu.VMEM((3 * spheres, 2, count * blocks, n), bf16), table, table]
        buffers.append(pltpu.SemaphoreType.DMA((2,)))
        return near_work(pieces, buffers)

    def near_work(pieces, buffers):
        gathered = call(gather_body, sources, [HB, HB] + [VM] * (2 * blocks), buffers)(
            *in_hbm((pair_shift, pair_member)), *pieces
        )
        return jnp.einsum(
            "ikarc,ikzcn->ikazrn", translation, gathered, preferred_element_type=f32
        )

    operands = (x, plane, wave_index.T, positions, ewald_weight.reshape(1, waves), mie_coef)
    buffers = [pltpu.VMEM(v.shape, v.dtype) for v in operands]
    buffers += [pltpu.VMEM((held_rows, waves), f32), pltpu.SemaphoreType.DMA((len(operands),))]
    rounded, send, keep, columns, plane = call(
        first_sums_body, (field_half, sums_half, sums, column, part), [HB] * len(operands), buffers
    )(*in_hbm(operands))
    mine, other = total_sums(send, keep)
    near = near_products(rounded)
    image, image_rounded, send, keep = call(
        first_image_body, (field, field_half, sums_half, sums), [VM] * 5
    )(near, mine, other, columns, plane)
    mine, other = total_sums(send, keep)
    near = near_products(image_rounded)
    image_two, gram = call(second_image_body, (field, shape((16, n))), [VM] * 7)(
        near, mine, other, columns, plane, x, image
    )
    gram = total_gram(gram)
    flat = shape((spheres, 2 * count, n))
    basis, residual, hessenberg = call(
        lambda *refs: finish_body(float(entries), *refs), (flat, flat, shape((9, n))), [VM] * 4
    )(gram, x, image, image_two)

    def unflatten(value):
        return value.reshape(spheres, count, 2, n).transpose(0, 2, 1, 3)

    return unflatten(basis), unflatten(residual), hessenberg


def solution(mesh):
    placed = (
        P("slab", None, "blk", None),
        P("slab", None, "blk"),
        P("slab", None, None, "blk", None),
        P("slab", None),
        P("slab", None),
        P("slab", None),
        P(),
        P(),
        P(),
    )
    return jax.shard_map(
        per_device,
        mesh=mesh,
        in_specs=placed,
        out_specs=(P("slab", None, "blk", None), P("slab", None, "blk", None), P()),
        check_vma=False,
    )
```

```python
import jax
import jax.numpy as jnp
from jax import lax
from jax.experimental import pallas as pl
from jax.experimental.pallas import tpu as pltpu
from jax.sharding import PartitionSpec as P

two_pi = 6.283185307179586
epsilon = 1e-06
f32 = jnp.float32
bf16 = jnp.bfloat16

VM = pl.BlockSpec(memory_space=pltpu.VMEM)
SM = pl.BlockSpec(memory_space=pltpu.SMEM)
HB = pl.BlockSpec(memory_space=pltpu.HBM)


def call(body, outs, specs, scratch=()):
    return pl.pallas_call(
        body,
        out_shape=outs,
        in_specs=specs,
        out_specs=jax.tree.map(lambda _: VM, outs),
        scratch_shapes=scratch,
        compiler_params=pltpu.CompilerParams(vmem_limit_bytes=16 << 20),
    )


def in_hbm(arrays):
    return [pltpu.with_memory_space_constraint(v, pltpu.HBM) for v in arrays]


def shape(dims, dtype=f32):
    return jax.ShapeDtypeStruct(dims, dtype)


def project(field, plane_ref, columns, spheres):
    sum_re = sum_im = None
    lead = (((0,), (0,)), ((), ()))
    for s in range(len(field)):
        both = jnp.concatenate(field[s], axis=1)
        with_re = lax.dot_general(plane_ref[0], both, lead, preferred_element_type=f32)
        with_im = lax.dot_general(plane_ref[1], both, lead, preferred_element_type=f32)
        n = both.shape[1] // 2
        part_re = with_re[:, :n] - with_im[:, n:]
        part_im = with_re[:, n:] + with_im[:, :n]
        c, d = columns[:, s : s + 1], columns[:, spheres + s : spheres + s + 1]
        turn_re = c * part_re + d * part_im
        turn_im = c * part_im - d * part_re
        sum_re = turn_re if sum_re is None else sum_re + turn_re
        sum_im = turn_im if sum_im is None else sum_im + turn_im
    return sum_re, sum_im


def split_halves(sum_re, sum_im, send_ref, keep_ref):
    half = sum_re.shape[0] // 2
    odd = lax.rem(lax.axis_index("blk"), 2) == 1
    n = sum_re.shape[1]
    for z, part in enumerate((sum_re, sum_im)):
        low, high = part[:half], part[half:]
        at = slice(z * n, (z + 1) * n)
        send_ref[:, at] = jnp.where(odd, low, high).astype(bf16)
        keep_ref[:, at] = jnp.where(odd, high, low)


def first_sums_body(
    x_hbm, plane_hbm, wave_hbm, pos_hbm, weight_hbm, mie_hbm,
    round_ref, send_ref, keep_ref, column_ref, part_ref,
    x_ref, plane_ref, wave_ref, pos_ref, weight_ref, mie_ref, held, sems,
):
    moves = ((wave_hbm, wave_ref), (pos_hbm, pos_ref), (weight_hbm, weight_ref), (mie_hbm, mie_ref))
    moves += ((plane_hbm, plane_ref), (x_hbm, x_ref))
    copies = [pltpu.make_async_copy(*move, sems.at[i]) for i, move in enumerate(moves)]
    for copy in copies:
        copy.start()
    for copy in copies[:-2]:
        copy.wait()
    spheres, _, count, _ = round_ref.shape
    b = lax.axis_index("blk")
    turns = None
    for d in range(3):
        term = wave_ref[d : d + 1, :].astype(f32) * pos_ref[:, d : d + 1]
        turns = term if turns is None else turns + term
    angles = two_pi * (turns - jnp.floor(turns + 0.5))
    cos, sin = jnp.cos(angles), jnp.sin(angles)
    weight = weight_ref[...]
    held[...] = jnp.zeros_like(held)
    for i, value in enumerate((cos, sin, weight * cos, weight * sin)):
        held[i * spheres : (i + 1) * spheres, :] = value
    for s in range(spheres):
        for z in range(2):
            at = 4 * spheres + 2 * s + z
            held[at : at + 1, 0:count] = mie_ref[s, z : z + 1, :]
    columns = held[...].T
    column_ref[...] = columns
    copies[-2].wait()
    for a in range(2):
        part = plane_ref[a, 0:count, :]
        for p in range(1, plane_ref.shape[1] // count):
            part = jnp.where(b == p, plane_ref[a, p * count : (p + 1) * count, :], part)
        part_ref[a] = part
    copies[-1].wait()
    field = []
    for s in range(spheres):
        field.append([x_ref[s, pl.ds(z, count, stride=2), :].astype(bf16) for z in range(2)])
        round_ref[s, 0] = field[s][0]
        round_ref[s, 1] = field[s][1]
    split_halves(*project(field, part_ref, columns, spheres), send_ref, keep_ref)


def gather_body(shift_hbm, member_hbm, *refs):
    *piece_refs, out_ref, held, shift_ref, member_ref, sems = refs
    copies = [
        pltpu.make_async_copy(shift_hbm, shift_ref, sems.at[0]),
        pltpu.make_async_copy(member_hbm, member_ref, sems.at[1]),
    ]
    for copy in copies:
        copy.start()
    blocks = len(piece_refs) // 2
    near_refs, odd_refs = piece_refs[:blocks], piece_refs[blocks:]
    spheres, _, _, _ = odd_refs[0].shape
    b = lax.axis_index("blk")
    parity = lax.rem(lax.axis_index("slab"), 2)
    for slot in range(3):
        for s in range(spheres):
            for z in range(2):
                if slot < 2:
                    parts = [ref[slot, s, z] for ref in near_refs]
                else:
                    parts = [ref[s, z] for ref in odd_refs]
                bit = 1
                while bit < blocks:
                    swap = lax.rem(lax.div(b, bit), 2) == 1
                    parts = [
                        jnp.where(swap, parts[i ^ bit], parts[i]) for i in range(blocks)
                    ]
                    bit *= 2
                held[slot * spheres + s, z] = jnp.concatenate(parts, axis=0)
    for copy in copies:
        copy.wait()
    for i in range(out_ref.shape[0]):
        for k in range(out_ref.shape[1]):
            shift = shift_ref[i, k]
            forward = (shift == 1) == (parity == 0)
            slot = jnp.where(shift == 0, 0, jnp.where(forward, 1, 2))
            out_ref[i, k] = held[slot * spheres + member_ref[i, k]]


def far_half(sums_ref, upper, columns_ref, plane_ref, spheres):
    half, n = sums_ref.shape[0], sums_ref.shape[1] // 2
    rows = pl.ds(pl.multiple_of(upper * half, half), half)
    total_re, total_im = sums_ref[:, :n].astype(f32), sums_ref[:, n:].astype(f32)
    plane_re, plane_im = plane_ref[0, :, rows], plane_ref[1, :, rows]
    columns = columns_ref[rows, :]
    fields = []
    for s in range(spheres):
        at = 2 * spheres + s
        c, d = columns[:, at : at + 1], columns[:, at + spheres : at + spheres + 1]
        turned = jnp.concatenate(
            [c * total_re - d * total_im, c * total_im + d * total_re], axis=1
        ).astype(bf16)
        with_re = jnp.dot(plane_re, turned, preferred_element_type=f32)
        with_im = jnp.dot(plane_im, turned, preferred_element_type=f32)
        fields.append(
            (with_re[:, :n] + with_im[:, n:], with_re[:, n:] - with_im[:, :n])
        )
    return fields


def field_sum_body(near_ref, mine_ref, column_ref, plane_ref, out_ref):
    spheres, pairs = near_ref.shape[:2]
    odd = lax.rem(lax.axis_index("blk"), 2)
    far = far_half(mine_ref, odd, column_ref, plane_ref, spheres)
    for s in range(spheres):
        sum_re, sum_im = far[s]
        for k in range(pairs):
            sum_re = sum_re + (near_ref[s, k, 0, 0] - near_ref[s, k, 1, 1])
            sum_im = sum_im + (near_ref[s, k, 0, 1] + near_ref[s, k, 1, 0])
        out_ref[s, 0] = sum_re
        out_ref[s, 1] = sum_im


def image_fields(sum_ref, other_ref, column_ref, plane_ref):
    spheres, _, count, _ = sum_ref.shape
    odd = lax.rem(lax.axis_index("blk"), 2)
    far = far_half(other_ref, 1 - odd, column_ref, plane_ref, spheres)
    out = []
    for s in range(spheres):
        sum_re, sum_im = sum_ref[s, 0] + far[s][0], sum_ref[s, 1] + far[s][1]
        at = 4 * spheres + 2 * s
        m_re = column_ref[0:count, at : at + 1]
        m_im = column_ref[0:count, at + 1 : at + 2]
        out.append((m_re * sum_re - m_im * sum_im, m_re * sum_im + m_im * sum_re))
    return out


def first_image_body(
    sum_ref, other_ref, column_ref, plane_ref,
    image_ref, round_ref, send_ref, keep_ref,
):
    images = image_fields(sum_ref, other_ref, column_ref, plane_ref)
    field = []
    for s, (re, im) in enumerate(images):
        image_ref[s, 0] = re
        image_ref[s, 1] = im
        field.append([re.astype(bf16), im.astype(bf16)])
        round_ref[s, 0] = field[s][0]
        round_ref[s, 1] = field[s][1]
    sums = project(field, plane_ref, column_ref[...], len(images))
    split_halves(*sums, send_ref, keep_ref)


def second_image_body(
    sum_ref, other_ref, column_ref, plane_ref, x_ref, g_ref, image_ref, gram_ref,
):
    images = image_fields(sum_ref, other_ref, column_ref, plane_ref)
    count = g_ref.shape[2]
    sums = None
    for s, (re, im) in enumerate(images):
        image_ref[s, 0] = re
        image_ref[s, 1] = im
        x = (x_ref[s, pl.ds(0, count, stride=2), :], x_ref[s, pl.ds(1, count, stride=2), :])
        g = (g_ref[s, 0], g_ref[s, 1])
        h = (re, im)
        terms = [x[0] * x[0] + x[1] * x[1]]
        terms += [x[0] * g[0] + x[1] * g[1], x[0] * g[1] - x[1] * g[0]]
        terms += [g[0] * g[0] + g[1] * g[1]]
        terms += [x[0] * h[0] + x[1] * h[1], x[0] * h[1] - x[1] * h[0]]
        terms += [g[0] * h[0] + g[1] * h[1], g[0] * h[1] - g[1] * h[0]]
        terms += [h[0] * h[0] + h[1] * h[1]]
        rows = [jnp.sum(term, axis=0, keepdims=True) for term in terms]
        sums = rows if sums is None else [a + r for a, r in zip(sums, rows)]
    high = [row.astype(bf16).astype(f32) for row in sums]
    low = [row - part for row, part in zip(sums, high)]
    rest = jnp.zeros((gram_ref.shape[1] - 2 * len(sums), gram_ref.shape[2]), f32)
    both = jnp.concatenate(high + low + [rest], axis=0).astype(bf16)
    gram_ref[...] = jnp.broadcast_to(both[None], gram_ref.shape)


def times(a, b):
    return (a[0] * b[0] - a[1] * b[1], a[0] * b[1] + a[1] * b[0])


def conj_times(a, b):
    return (a[0] * b[0] + a[1] * b[1], a[0] * b[1] - a[1] * b[0])


def plus(*terms):
    return (sum(t[0] for t in terms), sum(t[1] for t in terms))


def scaled(a, r):
    return (a[0] * r, a[1] * r)


def finish_body(entries, gram_ref, x_ref, g_ref, h_ref, basis_ref, residual_ref, hess_ref):
    gram = jnp.sum(gram_ref[...].astype(f32), axis=0) / entries
    row = [gram[i : i + 1, :] + gram[9 + i : 10 + i, :] for i in range(9)]
    xx, gg, hh = row[0], row[3], row[8]
    xg, xh, gh = (row[1], row[2]), (row[4], row[5]), (row[6], row[7])
    square = xx + epsilon
    beta = jnp.sqrt(square)
    inv = 1.0 / beta
    h11 = ((xx - xg[0]) / square, -xg[1] / square)
    alpha = ((epsilon + xg[0]) / square * inv, xg[1] / square * inv)
    delta = -inv
    cross = alpha[0] * xg[0] + alpha[1] * xg[1]
    norm = (alpha[0] * alpha[0] + alpha[1] * alpha[1]) * xx + delta * delta * gg + 2.0 * delta * cross
    h21 = jnp.sqrt(jnp.maximum(norm, 0.0) + epsilon)
    a = (alpha[0] / h21, alpha[1] / h21)
    d = delta / h21
    b = (d - a[0], -a[1])
    h12 = scaled(plus(scaled(a, xx), times(b, xg), scaled(xh, -d)), inv)
    e = (a[0] - h12[0] * inv, a[1] - h12[1] * inv)
    with_x = plus(scaled(e, xx), times(b, xg), scaled(xh, -d))
    with_g = plus(times(e, (xg[0], -xg[1])), scaled(b, gg), scaled(gh, -d))
    h22 = plus(conj_times(a, with_x), scaled(with_g, d))
    c0 = plus(e, scaled(times(h22, a), -1.0))
    c1 = plus(b, scaled(h22, -d))
    c2 = -d
    last = (
        (c0[0] * c0[0] + c0[1] * c0[1]) * xx
        + (c1[0] * c1[0] + c1[1] * c1[1]) * gg
        + c2 * c2 * hh
        + 2.0 * times(conj_times(c0, c1), xg)[0]
        + 2.0 * c2 * conj_times(c0, xh)[0]
        + 2.0 * c2 * conj_times(c1, gh)[0]
    )
    h32 = jnp.sqrt(jnp.maximum(last, 0.0) + epsilon)
    for i, value in enumerate((beta, h11[0], h11[1], h21, h12[0], h12[1], h22[0], h22[1], h32)):
        hess_ref[i : i + 1, :] = value
    count = g_ref.shape[2]
    for s in range(g_ref.shape[0]):
        rows = [pl.ds(z, count, stride=2) for z in range(2)]
        x = (x_ref[s, rows[0], :], x_ref[s, rows[1], :])
        g = (g_ref[s, 0], g_ref[s, 1])
        h = (h_ref[s, 0], h_ref[s, 1])
        basis = plus(times(a, x), scaled(g, d))
        residual = plus(times(c0, x), times(c1, g), scaled(h, c2))
        for z in range(2):
            basis_ref[s, rows[z], :] = basis[z]
            residual_ref[s, rows[z], :] = residual[z]


def trade(value, axis, bit):
    return lax.ppermute(value, axis, [(i, i ^ bit) for i in range(lax.axis_size(axis))])


def trade_odd(value):
    count = lax.axis_size("slab")
    pairs = []
    for i in range(count):
        pairs.append((i, (i + 1) % count if i % 2 else (i - 1) % count))
    return lax.ppermute(value, "slab", pairs)


def bits(axis, start=1):
    out, bit = [], start
    while bit < lax.axis_size(axis):
        out.append(bit)
        bit *= 2
    return out


def fetch_pieces(own):
    out = []
    even = trade(own, "slab", 1)
    groups = [jnp.stack([own, even]), trade_odd(own)]
    for group in groups:
        pieces = {0: group}
        for bit in bits("blk", 2):
            pieces.update({r | bit: trade(value, "blk", bit) for r, value in list(pieces.items())})
        for r, value in list(pieces.items()):
            pieces[r | 1] = trade(value, "blk", 1)
        out += [pieces[r] for r in range(len(pieces))]
    return out


def total_sums(send, keep):
    keep = keep + trade(send, "blk", 1).astype(f32)
    steps = [("blk", bit) for bit in bits("blk", 2)] + [("slab", bit) for bit in bits("slab")]
    steps[1:3] = steps[2:0:-1]
    for axis, bit in steps:
        keep = keep + trade(keep.astype(bf16), axis, bit).astype(f32)
    return keep, trade(keep.astype(bf16), "blk", 1)


def per_device(
    incident, mie_coef, translation, pair_shift, pair_member, positions, wave_index, plane_coef,
    ewald_weight,
):
    spheres, _, count, n = incident.shape
    pairs = translation.shape[1]
    blocks = lax.axis_size("blk")
    waves = plane_coef.shape[0]
    entries = spheres * lax.axis_size("slab") * count * blocks
    x = incident.transpose(0, 2, 1, 3).reshape(spheres, 2 * count, n)
    plane = plane_coef.transpose(1, 2, 0)

    field = shape((spheres, 2, count, n))
    field_half = shape((spheres, 2, count, n), bf16)
    sums = shape((waves // 2, 2 * n))
    sums_half = shape((waves // 2, 2 * n), bf16)
    sources = shape((spheres, pairs, 2, count * blocks, n), bf16)
    held_rows = -(-6 * spheres // 8) * 8
    column = shape((waves, held_rows))
    part = shape((2, count, waves), bf16)

    def near_products(own):
        pieces = fetch_pieces(own)
        table = pltpu.SMEM((spheres, pairs), jnp.int32)
        buffers = [pltpu.VMEM((3 * spheres, 2, count * blocks, n), bf16), table, table]
        buffers.append(pltpu.SemaphoreType.DMA((2,)))
        return near_work(pieces, buffers)

    def near_work(pieces, buffers):
        gathered = call(gather_body, sources, [HB, HB] + [VM] * (2 * blocks), buffers)(
            *in_hbm((pair_shift, pair_member)), *pieces
        )
        return jnp.einsum(
            "ikarc,ikzcn->ikazrn", translation, gathered, preferred_element_type=f32
        )

    def both_fields(own, send, keep, columns, plane):
        mine, other = total_sums(send, keep)
        near = near_products(own)
        field_sums = call(field_sum_body, field, [VM] * 4)(near, mine, columns, plane)
        return field_sums, other

    operands = (x, plane, wave_index.T, positions, ewald_weight.reshape(1, waves), mie_coef)
    buffers = [pltpu.VMEM(v.shape, v.dtype) for v in operands]
    buffers += [pltpu.VMEM((held_rows, waves), f32), pltpu.SemaphoreType.DMA((len(operands),))]
    rounded, send, keep, columns, plane = call(
        first_sums_body, (field_half, sums_half, sums, column, part), [HB] * len(operands), buffers
    )(*in_hbm(operands))
    field_sums, other = both_fields(rounded, send, keep, columns, plane)
    image, image_rounded, send, keep = call(
        first_image_body, (field, field_half, sums_half, sums), [VM] * 4
    )(field_sums, other, columns, plane)
    field_sums, other = both_fields(image_rounded, send, keep, columns, plane)
    devices = blocks * lax.axis_size("slab")
    image_two, gram = call(
        second_image_body, (field, shape((devices, 24, n), bf16)), [VM] * 6
    )(field_sums, other, columns, plane, x, image)
    gram = lax.all_to_all(gram, ("slab", "blk"), 0, 0, tiled=True)
    flat = shape((spheres, 2 * count, n))
    basis, residual, hessenberg = call(
        lambda *refs: finish_body(float(entries), *refs), (flat, flat, shape((9, n))), [VM] * 4
    )(gram, x, image, image_two)

    def unflatten(value):
        return value.reshape(spheres, count, 2, n).transpose(0, 2, 1, 3)

    return unflatten(basis), unflatten(residual), hessenberg


def solution(mesh):
    placed = (
        P("slab", None, "blk", None),
        P("slab", None, "blk"),
        P("slab", None, None, "blk", None),
        P("slab", None),
        P("slab", None),
        P("slab", None),
        P(),
        P(),
        P(),
    )
    return jax.shard_map(
        per_device,
        mesh=mesh,
        in_specs=placed,
        out_specs=(P("slab", None, "blk", None), P("slab", None, "blk", None), P()),
        check_vma=False,
    )
```

```python
import jax
import jax.numpy as jnp
from jax import lax
from jax.experimental import pallas as pl
from jax.experimental.layout import Layout, with_layout_constraint
from jax.experimental.pallas import tpu as pltpu
from jax.sharding import PartitionSpec as P

two_pi = 6.283185307179586
epsilon = 1e-06
f32 = jnp.float32
bf16 = jnp.bfloat16

VM = pl.BlockSpec(memory_space=pltpu.VMEM)
SM = pl.BlockSpec(memory_space=pltpu.SMEM)
HB = pl.BlockSpec(memory_space=pltpu.HBM)


def call(body, outs, specs, scratch=()):
    return pl.pallas_call(
        body,
        out_shape=outs,
        in_specs=specs,
        out_specs=jax.tree.map(lambda _: VM, outs),
        scratch_shapes=scratch,
        compiler_params=pltpu.CompilerParams(vmem_limit_bytes=16 << 20),
    )


def in_hbm(arrays):
    return [pltpu.with_memory_space_constraint(v, pltpu.HBM) for v in arrays]


def shape(dims, dtype=f32):
    return jax.ShapeDtypeStruct(dims, dtype)


def turn(value):
    half = value.shape[1] // 2
    lane = lax.broadcasted_iota(jnp.int32, (1, 2 * half), 1)
    return pltpu.roll(value, half, 1) * jnp.where(lane < half, -1.0, 1.0)


def second():
    return lax.rem(lax.axis_index("blk"), 2) == 1


def split_body(x_hbm, send_ref, keep_ref, x_ref, sem):
    copy = pltpu.make_async_copy(x_hbm, x_ref, sem)
    copy.start()
    copy.wait()
    spheres, count, n = keep_ref.shape
    half = n // 2
    for s in range(spheres):
        re, im = (x_ref[s, pl.ds(z, count, stride=2), :] for z in range(2))
        low = jnp.concatenate([re[:, :half], im[:, :half]], axis=1)
        high = jnp.concatenate([re[:, half:], im[:, half:]], axis=1)
        send_ref[s] = jnp.where(second(), low, high)
        keep_ref[s] = jnp.where(second(), high, low)


def tables_body(
    mie_other_ref, plane_hbm, wave_hbm, pos_hbm, weight_hbm, mie_hbm,
    column_ref, part_ref, plane_ref, wave_ref, pos_ref, weight_ref, mie_ref, held, sems,
):
    moves = ((wave_hbm, wave_ref), (pos_hbm, pos_ref), (weight_hbm, weight_ref), (mie_hbm, mie_ref))
    moves += ((plane_hbm, plane_ref),)
    copies = [pltpu.make_async_copy(*move, sems.at[i]) for i, move in enumerate(moves)]
    for copy in copies:
        copy.start()
    for copy in copies[:-1]:
        copy.wait()
    spheres, _, count = mie_ref.shape
    b = lax.axis_index("blk")
    turns = None
    for d in range(3):
        term = wave_ref[d : d + 1, :].astype(f32) * pos_ref[:, d : d + 1]
        turns = term if turns is None else turns + term
    angles = two_pi * (turns - jnp.floor(turns + 0.5))
    cos, sin = jnp.cos(angles), jnp.sin(angles)
    weight = weight_ref[...]
    held[...] = jnp.zeros_like(held)
    for i, value in enumerate((cos, sin, weight * cos, weight * sin)):
        held[i * spheres : (i + 1) * spheres, :] = value
    for o, ref in enumerate((mie_ref, mie_other_ref)):
        for s in range(spheres):
            for z in range(2):
                at = 4 * spheres + 2 * (o * spheres + s) + z
                held[at : at + 1, 0:count] = ref[s, z : z + 1, :]
    column_ref[...] = held[...].T
    copies[-1].wait()
    mate = b + 1 - 2 * lax.rem(b, 2)
    for o, block in enumerate((b, mate)):
        for a in range(2):
            part = plane_ref[a, 0:count, :]
            for p in range(1, plane_ref.shape[1] // count):
                part = jnp.where(block == p, plane_ref[a, p * count : (p + 1) * count, :], part)
            part_ref[o, a] = part


def project(field, part_ref, columns, spheres):
    total = None
    lead = (((0,), (0,)), ((), ()))
    with_re = with_im = None
    for o in range(2):
        side = jnp.concatenate([field[s][o] for s in range(spheres)], axis=1)
        one = lax.dot_general(part_ref[o, 0], side, lead, preferred_element_type=f32)
        two = lax.dot_general(part_ref[o, 1], side, lead, preferred_element_type=f32)
        with_re = one if with_re is None else with_re + one
        with_im = two if with_im is None else with_im + two
    n = with_re.shape[1] // spheres
    for s in range(spheres):
        at = slice(s * n, (s + 1) * n)
        part = with_re[:, at] + turn(with_im[:, at])
        c, d = columns[:, s : s + 1], columns[:, spheres + s : spheres + s + 1]
        value = c * part - d * turn(part)
        total = value if total is None else total + value
    return total


def put_rounded(round_ref, s, mine, other):
    first = jnp.where(second(), other, mine)
    last = jnp.where(second(), mine, other)
    round_ref[s] = jnp.concatenate([first, last], axis=0).astype(bf16)


def first_sums_body(mine_ref, other_ref, column_ref, part_ref, round_ref, send_ref, keep_ref):
    spheres = mine_ref.shape[0]
    field = []
    for s in range(spheres):
        put_rounded(round_ref, s, mine_ref[s], other_ref[s])
        field.append([mine_ref[s].astype(bf16), other_ref[s].astype(bf16)])
    total = project(field, part_ref, column_ref[...], spheres)
    keep_ref[...] = total
    send_ref[...] = total.astype(bf16)


def gather_body(shift_hbm, member_hbm, *refs):
    *piece_refs, out_ref, held, shift_ref, member_ref, sems = refs
    copies = [
        pltpu.make_async_copy(shift_hbm, shift_ref, sems.at[0]),
        pltpu.make_async_copy(member_hbm, member_ref, sems.at[1]),
    ]
    for copy in copies:
        copy.start()
    groups = len(piece_refs) // 2
    near_refs, odd_refs = piece_refs[:groups], piece_refs[groups:]
    spheres = odd_refs[0].shape[0]
    place = lax.div(lax.axis_index("blk"), 2)
    parity = lax.rem(lax.axis_index("slab"), 2)
    for slot in range(3):
        for s in range(spheres):
            parts = [ref[slot, s] for ref in near_refs] if slot < 2 else [ref[s] for ref in odd_refs]
            bit = 1
            while bit < groups:
                swap = lax.rem(lax.div(place, bit), 2) == 1
                parts = [jnp.where(swap, parts[i ^ bit], parts[i]) for i in range(groups)]
                bit *= 2
            held[slot * spheres + s] = jnp.concatenate(parts, axis=0)
    for copy in copies:
        copy.wait()
    for i in range(out_ref.shape[0]):
        for k in range(out_ref.shape[1]):
            shift = shift_ref[i, k]
            forward = (shift == 1) == (parity == 0)
            slot = jnp.where(shift == 0, 0, jnp.where(forward, 1, 2))
            out_ref[i, k] = held[slot * spheres + member_ref[i, k]]


def near_sum_body(mine_ref, other_ref, out_ref):
    spheres, pairs = mine_ref.shape[:2]
    for o, ref in enumerate((mine_ref, other_ref)):
        for s in range(spheres):
            with_re, with_im = ref[s, 0, 0], ref[s, 0, 1]
            for k in range(1, pairs):
                with_re = with_re + ref[s, k, 0]
                with_im = with_im + ref[s, k, 1]
            out_ref[o, s] = with_re + turn(with_im)


def image_fields(near_ref, total_ref, column_ref, part_ref):
    _, spheres, count, _ = near_ref.shape
    columns, total = column_ref[...], total_ref[...]
    turned_total = turn(total)
    sides = []
    for s in range(spheres):
        at = 2 * spheres + s
        c, d = columns[:, at : at + 1], columns[:, at + spheres : at + spheres + 1]
        sides.append((c * total + d * turned_total).astype(bf16))
    turned = jnp.concatenate(sides, axis=1)
    n = total.shape[1]
    out = [[] for _ in range(spheres)]
    for o in range(2):
        with_re = jnp.dot(part_ref[o, 0], turned, preferred_element_type=f32)
        with_im = jnp.dot(part_ref[o, 1], turned, preferred_element_type=f32)
        for s in range(spheres):
            at = slice(s * n, (s + 1) * n)
            value = near_ref[o, s] + with_re[:, at] - turn(with_im[:, at])
            at = 4 * spheres + 2 * (o * spheres + s)
            m_re, m_im = column_ref[0:count, at : at + 1], column_ref[0:count, at + 1 : at + 2]
            out[s].append(m_re * value + m_im * turn(value))
    return out


def first_image_body(
    near_ref, total_ref, column_ref, part_ref, mine_ref, other_ref, round_ref, send_ref, keep_ref
):
    images = image_fields(near_ref, total_ref, column_ref, part_ref)
    field = []
    for s, (mine, other) in enumerate(images):
        mine_ref[s] = mine
        other_ref[s] = other
        put_rounded(round_ref, s, mine, other)
        field.append([mine.astype(bf16), other.astype(bf16)])
    total = project(field, part_ref, column_ref[...], len(images))
    keep_ref[...] = total
    send_ref[...] = total.astype(bf16)


def second_image_body(
    near_ref, total_ref, column_ref, part_ref, x_ref, x_other_ref, g_ref, g_other_ref,
    mine_ref, other_ref, gram_ref,
):
    images = image_fields(near_ref, total_ref, column_ref, part_ref)
    half = total_ref.shape[1] // 2
    sums = None
    for s, rows in enumerate(images):
        mine_ref[s] = rows[0]
        other_ref[s] = rows[1]
        for x, g, h in ((x_ref[s], g_ref[s], rows[0]), (x_other_ref[s], g_other_ref[s], rows[1])):
            tx, tg = turn(x), turn(g)
            terms = (x * x, x * g, tx * g, g * g, x * h, tx * h, g * h, tg * h, h * h)
            found = [jnp.sum(term, axis=0, keepdims=True) for term in terms]
            sums = found if sums is None else [a + r for a, r in zip(sums, found)]
    sums = [row[:, :half] + row[:, half:] for row in sums] + [jnp.zeros((1, half), f32)]
    rows = [jnp.concatenate(sums[i : i + 2], axis=1) for i in range(0, len(sums), 2)]
    rest = jnp.zeros((gram_ref.shape[1] - len(rows), 2 * half), f32)
    gram_ref[...] = jnp.broadcast_to(jnp.concatenate(rows + [rest], axis=0)[None], gram_ref.shape)


def times(a, b):
    return (a[0] * b[0] - a[1] * b[1], a[0] * b[1] + a[1] * b[0])


def conj_times(a, b):
    return (a[0] * b[0] + a[1] * b[1], a[0] * b[1] - a[1] * b[0])


def plus(*terms):
    return (sum(t[0] for t in terms), sum(t[1] for t in terms))


def scaled(a, r):
    return (a[0] * r, a[1] * r)


def finish_body(
    entries, gram_ref, x_ref, g_ref, g_other_ref, h_ref, h_other_ref, basis_ref, residual_ref, hess_ref
):
    devices = gram_ref.shape[0]
    parts = [gram_ref[i] for i in range(2)]
    for i in range(2, devices):
        parts[i % 2] = parts[i % 2] + gram_ref[i]
    low, high = (part / entries for part in parts)
    half = low.shape[1] // 2
    row = []
    for i in range(9):
        at = (slice(i // 2, i // 2 + 1), slice(i % 2 * half, (i % 2 + 1) * half))
        row.append(jnp.concatenate([low[at], high[at]], axis=1))
    xx, gg, hh = row[0], row[3], row[8]
    xg, xh, gh = (row[1], row[2]), (row[4], row[5]), (row[6], row[7])
    square = xx + epsilon
    beta = jnp.sqrt(square)
    inv = 1.0 / beta
    h11 = ((xx - xg[0]) / square, -xg[1] / square)
    alpha = ((epsilon + xg[0]) / square * inv, xg[1] / square * inv)
    delta = -inv
    cross = alpha[0] * xg[0] + alpha[1] * xg[1]
    norm = (alpha[0] * alpha[0] + alpha[1] * alpha[1]) * xx + delta * delta * gg + 2.0 * delta * cross
    h21 = jnp.sqrt(jnp.maximum(norm, 0.0) + epsilon)
    a = (alpha[0] / h21, alpha[1] / h21)
    d = delta / h21
    b = (d - a[0], -a[1])
    h12 = scaled(plus(scaled(a, xx), times(b, xg), scaled(xh, -d)), inv)
    e = (a[0] - h12[0] * inv, a[1] - h12[1] * inv)
    with_x = plus(scaled(e, xx), times(b, xg), scaled(xh, -d))
    with_g = plus(times(e, (xg[0], -xg[1])), scaled(b, gg), scaled(gh, -d))
    h22 = plus(conj_times(a, with_x), scaled(with_g, d))
    c0 = plus(e, scaled(times(h22, a), -1.0))
    c1 = plus(b, scaled(h22, -d))
    c2 = -d
    last = (
        (c0[0] * c0[0] + c0[1] * c0[1]) * xx
        + (c1[0] * c1[0] + c1[1] * c1[1]) * gg
        + c2 * c2 * hh
        + 2.0 * times(conj_times(c0, c1), xg)[0]
        + 2.0 * c2 * conj_times(c0, xh)[0]
        + 2.0 * c2 * conj_times(c1, gh)[0]
    )
    h32 = jnp.sqrt(jnp.maximum(last, 0.0) + epsilon)
    for i, value in enumerate((beta, h11[0], h11[1], h21, h12[0], h12[1], h22[0], h22[1], h32)):
        hess_ref[i : i + 1, :] = value
    count = g_ref.shape[1]

    def whole(mine, other):
        low, high = jnp.where(second(), other, mine), jnp.where(second(), mine, other)
        return tuple(
            jnp.concatenate([low[:, at : at + half], high[:, at : at + half]], axis=1) for at in (0, half)
        )

    for s in range(g_ref.shape[0]):
        rows = [pl.ds(z, count, stride=2) for z in range(2)]
        x = (x_ref[s, rows[0], :], x_ref[s, rows[1], :])
        g = whole(g_ref[s], g_other_ref[s])
        h = whole(h_ref[s], h_other_ref[s])
        basis = plus(times(a, x), scaled(g, d))
        residual = plus(times(c0, x), times(c1, g), scaled(h, c2))
        for z in range(2):
            basis_ref[s, rows[z], :] = basis[z]
            residual_ref[s, rows[z], :] = residual[z]


def trade(value, axis, bit):
    return lax.ppermute(value, axis, [(i, i ^ bit) for i in range(lax.axis_size(axis))])


def trade_odd(value):
    count = lax.axis_size("slab")
    pairs = []
    for i in range(count):
        pairs.append((i, (i + 1) % count if i % 2 else (i - 1) % count))
    return lax.ppermute(value, "slab", pairs)


def bits(axis, start=1):
    out, bit = [], start
    while bit < lax.axis_size(axis):
        out.append(bit)
        bit *= 2
    return out


def fetch_pieces(own):
    out = []
    even = trade(own, "slab", 1)
    groups = [jnp.stack([own, even]), trade_odd(own)]
    for group in groups:
        pieces = {0: group}
        for bit in bits("blk", 2):
            pieces.update({r | bit // 2: trade(value, "blk", bit) for r, value in list(pieces.items())})
        out += [pieces[r] for r in range(len(pieces))]
    return out


def total_sums(send, keep):
    steps = [("blk", bit) for bit in bits("blk", 2)] + [("slab", bit) for bit in bits("slab")]
    steps[1:3] = steps[2:0:-1]
    for axis, bit in steps:
        keep = keep + trade(send, axis, bit).astype(f32)
        send = keep.astype(bf16)
    return keep


def per_device(
    incident, mie_coef, translation, pair_shift, pair_member, positions, wave_index, plane_coef,
    ewald_weight,
):
    spheres, _, count, n = incident.shape
    pairs = translation.shape[1]
    blocks = lax.axis_size("blk")
    devices = blocks * lax.axis_size("slab")
    waves = plane_coef.shape[0]
    entries = spheres * lax.axis_size("slab") * count * blocks
    x = incident.transpose(0, 2, 1, 3).reshape(spheres, 2 * count, n)

    field = shape((spheres, count, n))
    both = shape((2, spheres, count, n))
    pair_half = shape((spheres, 2 * count, n), bf16)
    sums = shape((waves, n))
    sums_half = shape((waves, n), bf16)
    sources = shape((spheres, pairs, count * blocks, n), bf16)
    held_rows = -(-8 * spheres // 8) * 8
    column = shape((waves, held_rows))
    part = shape((2, 2, count, waves), bf16)

    def both_fields(own, send, keep):
        total = total_sums(send, keep)
        pieces = fetch_pieces(own)
        table = pltpu.SMEM((spheres, pairs), jnp.int32)
        buffers = [pltpu.VMEM((3 * spheres, count * blocks, n), bf16), table, table]
        buffers.append(pltpu.SemaphoreType.DMA((2,)))
        gathered = call(gather_body, sources, [HB, HB] + [VM] * blocks, buffers)(
            *in_hbm((pair_shift, pair_member)), *pieces
        )
        products = [
            jnp.einsum("ikarc,ikcn->ikarn", rows, gathered, preferred_element_type=f32)
            for rows in (rows_mine, rows_other)
        ]
        near = call(near_sum_body, both, [VM] * 2)(*products)
        return near, total

    mie_other = trade(mie_coef, "blk", 1)
    buffers = [pltpu.VMEM(x.shape, f32), pltpu.SemaphoreType.DMA]
    send, x_mine = call(split_body, (field, field), [HB], buffers)(*in_hbm([x]))
    x_other = trade(send, "blk", 1)
    stored = Layout(major_to_minor=(0, 1, 3, 2, 4))
    rows_mine = with_layout_constraint(translation, stored)
    operands = (
        plane_coef.transpose(1, 2, 0), wave_index.T, positions, ewald_weight.reshape(1, waves), mie_coef
    )
    buffers = [pltpu.VMEM(v.shape, v.dtype) for v in operands]
    buffers += [pltpu.VMEM((held_rows, waves), f32), pltpu.SemaphoreType.DMA((len(operands),))]
    columns, plane = call(
        tables_body, (column, part), [VM] + [HB] * len(operands), buffers
    )(mie_other, *in_hbm(operands))
    rounded, send, keep = call(first_sums_body, (pair_half, sums_half, sums), [VM] * 4)(x_mine, x_other, columns, plane)
    rows_other = with_layout_constraint(trade(rows_mine, "blk", 1), stored)
    near, total = both_fields(rounded, send, keep)
    g_mine, g_other, rounded, send, keep = call(
        first_image_body, (field, field, pair_half, sums_half, sums), [VM] * 4
    )(near, total, columns, plane)
    g_back = trade(g_other, "blk", 1)
    near, total = both_fields(rounded, send, keep)
    h_mine, h_other, gram = call(
        second_image_body, (field, field, shape((devices, 8, n))), [VM] * 8
    )(near, total, columns, plane, x_mine, x_other, g_mine, g_other)
    h_back = trade(h_other, "blk", 1)
    gram = lax.all_to_all(gram, ("slab", "blk"), 0, 0, tiled=True)
    flat = shape((spheres, 2 * count, n))
    basis, residual, hessenberg = call(
        lambda *refs: finish_body(float(entries), *refs), (flat, flat, shape((9, n))), [VM] * 6
    )(gram, x, g_mine, g_back, h_mine, h_back)

    def unflatten(value):
        return value.reshape(spheres, count, 2, n).transpose(0, 2, 1, 3)

    return unflatten(basis), unflatten(residual), hessenberg


def solution(mesh):
    placed = (
        P("slab", None, "blk", None),
        P("slab", None, "blk"),
        P("slab", None, None, "blk", None),
        P("slab", None),
        P("slab", None),
        P("slab", None),
        P(),
        P(),
        P(),
    )
    return jax.shard_map(
        per_device,
        mesh=mesh,
        in_specs=placed,
        out_specs=(P("slab", None, "blk", None), P("slab", None, "blk", None), P()),
        check_vma=False,
    )
```

```python
import jax
import jax.numpy as jnp
from jax import lax
from jax.experimental import pallas as pl
from jax.experimental.layout import Layout, with_layout_constraint
from jax.experimental.pallas import tpu as pltpu
from jax.sharding import PartitionSpec as P

two_pi = 6.283185307179586
epsilon = 1e-06
f32 = jnp.float32
bf16 = jnp.bfloat16

VM = pl.BlockSpec(memory_space=pltpu.VMEM)
SM = pl.BlockSpec(memory_space=pltpu.SMEM)
HB = pl.BlockSpec(memory_space=pltpu.HBM)


def call(body, outs, specs, scratch=()):
    return pl.pallas_call(
        body,
        out_shape=outs,
        in_specs=specs,
        out_specs=jax.tree.map(lambda _: VM, outs),
        scratch_shapes=scratch,
        compiler_params=pltpu.CompilerParams(vmem_limit_bytes=16 << 20),
    )


def in_hbm(arrays):
    return [pltpu.with_memory_space_constraint(v, pltpu.HBM) for v in arrays]


def shape(dims, dtype=f32):
    return jax.ShapeDtypeStruct(dims, dtype)


def turn(value):
    half = value.shape[1] // 2
    lane = lax.broadcasted_iota(jnp.int32, (1, 2 * half), 1)
    return pltpu.roll(value, half, 1) * jnp.where(lane < half, -1.0, 1.0)


def second():
    return lax.rem(lax.axis_index("blk"), 2) == 1


def split_body(x_hbm, send_ref, keep_ref, x_ref, sem):
    copy = pltpu.make_async_copy(x_hbm, x_ref, sem)
    copy.start()
    copy.wait()
    spheres, count, n = keep_ref.shape
    half = n // 2
    for s in range(spheres):
        re, im = (x_ref[s, pl.ds(z, count, stride=2), :] for z in range(2))
        low = jnp.concatenate([re[:, :half], im[:, :half]], axis=1)
        high = jnp.concatenate([re[:, half:], im[:, half:]], axis=1)
        send_ref[s] = jnp.where(second(), low, high)
        keep_ref[s] = jnp.where(second(), high, low)


def tables_body(
    mie_other_ref, plane_hbm, wave_hbm, pos_hbm, weight_hbm, mie_hbm,
    column_ref, part_ref, plane_ref, wave_ref, pos_ref, weight_ref, mie_ref, held, sems,
):
    moves = ((wave_hbm, wave_ref), (pos_hbm, pos_ref), (weight_hbm, weight_ref), (mie_hbm, mie_ref))
    moves += ((plane_hbm, plane_ref),)
    copies = [pltpu.make_async_copy(*move, sems.at[i]) for i, move in enumerate(moves)]
    for copy in copies:
        copy.start()
    for copy in copies[:-1]:
        copy.wait()
    spheres, _, count = mie_ref.shape
    b = lax.axis_index("blk")
    turns = None
    for d in range(3):
        term = wave_ref[d : d + 1, :].astype(f32) * pos_ref[:, d : d + 1]
        turns = term if turns is None else turns + term
    angles = two_pi * (turns - jnp.floor(turns + 0.5))
    cos, sin = jnp.cos(angles), jnp.sin(angles)
    weight = weight_ref[...]
    held[...] = jnp.zeros_like(held)
    for i, value in enumerate((cos, sin, weight * cos, weight * sin)):
        held[i * spheres : (i + 1) * spheres, :] = value
    for o, ref in enumerate((mie_ref, mie_other_ref)):
        for s in range(spheres):
            for z in range(2):
                at = 4 * spheres + 2 * (o * spheres + s) + z
                held[at : at + 1, 0:count] = ref[s, z : z + 1, :]
    column_ref[...] = held[...].T
    copies[-1].wait()
    mate = b + 1 - 2 * lax.rem(b, 2)
    for o, block in enumerate((b, mate)):
        for a in range(2):
            part = plane_ref[a, 0:count, :]
            for p in range(1, plane_ref.shape[1] // count):
                part = jnp.where(block == p, plane_ref[a, p * count : (p + 1) * count, :], part)
            part_ref[o, a] = part


def spread_body(column_ref, wide_ref, wide_mie_ref):
    for i in range(wide_ref.shape[0]):
        wide_ref[i] = jnp.broadcast_to(column_ref[:, i : i + 1], wide_ref.shape[1:])
    count = wide_mie_ref.shape[1]
    for i in range(wide_mie_ref.shape[0]):
        at = wide_ref.shape[0] + i
        wide_mie_ref[i] = jnp.broadcast_to(column_ref[0:count, at : at + 1], wide_mie_ref.shape[1:])


def project(field, part_ref, column, spheres):
    total = None
    lead = (((0,), (0,)), ((), ()))
    with_re = with_im = None
    for o in range(2):
        side = jnp.concatenate([field[s][o] for s in range(spheres)], axis=1)
        one = lax.dot_general(part_ref[o, 0], side, lead, preferred_element_type=f32)
        two = lax.dot_general(part_ref[o, 1], side, lead, preferred_element_type=f32)
        with_re = one if with_re is None else with_re + one
        with_im = two if with_im is None else with_im + two
    n = with_re.shape[1] // spheres
    for s in range(spheres):
        at = slice(s * n, (s + 1) * n)
        part = with_re[:, at] + turn(with_im[:, at])
        c, d = column(s), column(spheres + s)
        value = c * part - d * turn(part)
        total = value if total is None else total + value
    return total


def put_rounded(round_ref, s, mine, other):
    first = jnp.where(second(), other, mine)
    last = jnp.where(second(), mine, other)
    round_ref[s] = jnp.concatenate([first, last], axis=0).astype(bf16)


def first_sums_body(mine_ref, other_ref, column_ref, part_ref, round_ref, send_ref, keep_ref):
    spheres = mine_ref.shape[0]
    field = []
    for s in range(spheres):
        put_rounded(round_ref, s, mine_ref[s], other_ref[s])
        field.append([mine_ref[s].astype(bf16), other_ref[s].astype(bf16)])
    total = project(field, part_ref, lambda i: column_ref[:, i : i + 1], spheres)
    keep_ref[...] = total
    send_ref[...] = total.astype(bf16)


def gather_body(shift_hbm, member_hbm, *refs):
    *piece_refs, out_ref, held, shift_ref, member_ref, sems = refs
    copies = [
        pltpu.make_async_copy(shift_hbm, shift_ref, sems.at[0]),
        pltpu.make_async_copy(member_hbm, member_ref, sems.at[1]),
    ]
    for copy in copies:
        copy.start()
    groups = len(piece_refs) // 2
    near_refs, odd_refs = piece_refs[:groups], piece_refs[groups:]
    spheres = odd_refs[0].shape[0]
    place = lax.div(lax.axis_index("blk"), 2)
    parity = lax.rem(lax.axis_index("slab"), 2)
    for slot in range(3):
        for s in range(spheres):
            parts = [ref[slot, s] for ref in near_refs] if slot < 2 else [ref[s] for ref in odd_refs]
            bit = 1
            while bit < groups:
                swap = lax.rem(lax.div(place, bit), 2) == 1
                parts = [jnp.where(swap, parts[i ^ bit], parts[i]) for i in range(groups)]
                bit *= 2
            held[slot * spheres + s] = jnp.concatenate(parts, axis=0)
    for copy in copies:
        copy.wait()
    for i in range(out_ref.shape[0]):
        for k in range(out_ref.shape[1]):
            shift = shift_ref[i, k]
            forward = (shift == 1) == (parity == 0)
            slot = jnp.where(shift == 0, 0, jnp.where(forward, 1, 2))
            out_ref[i, k] = held[slot * spheres + member_ref[i, k]]


def near_sum_body(mine_ref, other_ref, out_ref):
    spheres, pairs = mine_ref.shape[:2]
    for o, ref in enumerate((mine_ref, other_ref)):
        for s in range(spheres):
            with_re, with_im = ref[s, 0, 0], ref[s, 0, 1]
            for k in range(1, pairs):
                with_re = with_re + ref[s, k, 0]
                with_im = with_im + ref[s, k, 1]
            out_ref[o, s] = with_re + turn(with_im)


def image_fields(near_ref, total_ref, wide_ref, wide_mie_ref, part_ref):
    spheres = near_ref.shape[1]
    total = total_ref[...]
    turned_total = turn(total)
    sides = []
    for s in range(spheres):
        at = 2 * spheres + s
        sides.append((wide_ref[at] * total + wide_ref[at + spheres] * turned_total).astype(bf16))
    turned = jnp.concatenate(sides, axis=1)
    n = total.shape[1]
    out = [[] for _ in range(spheres)]
    for o in range(2):
        with_re = jnp.dot(part_ref[o, 0], turned, preferred_element_type=f32)
        with_im = jnp.dot(part_ref[o, 1], turned, preferred_element_type=f32)
        for s in range(spheres):
            at = slice(s * n, (s + 1) * n)
            value = near_ref[o, s] + with_re[:, at] - turn(with_im[:, at])
            at = 2 * (o * spheres + s)
            m_re, m_im = wide_mie_ref[at], wide_mie_ref[at + 1]
            out[s].append(m_re * value + m_im * turn(value))
    return out


def first_image_body(
    near_ref, total_ref, wide_ref, wide_mie_ref, part_ref, mine_ref, other_ref, round_ref, send_ref, keep_ref
):
    images = image_fields(near_ref, total_ref, wide_ref, wide_mie_ref, part_ref)
    field = []
    for s, (mine, other) in enumerate(images):
        mine_ref[s] = mine
        other_ref[s] = other
        put_rounded(round_ref, s, mine, other)
        field.append([mine.astype(bf16), other.astype(bf16)])
    total = project(field, part_ref, lambda i: wide_ref[i], len(images))
    keep_ref[...] = total
    send_ref[...] = total.astype(bf16)


def second_image_body(
    near_ref, total_ref, wide_ref, wide_mie_ref, part_ref, x_ref, x_other_ref, g_ref, g_other_ref,
    mine_ref, other_ref, gram_ref,
):
    images = image_fields(near_ref, total_ref, wide_ref, wide_mie_ref, part_ref)
    half = total_ref.shape[1] // 2
    sums = None
    for s, rows in enumerate(images):
        mine_ref[s] = rows[0]
        other_ref[s] = rows[1]
        for x, g, h in ((x_ref[s], g_ref[s], rows[0]), (x_other_ref[s], g_other_ref[s], rows[1])):
            tx, tg = turn(x), turn(g)
            terms = (x * x, x * g, tx * g, g * g, x * h, tx * h, g * h, tg * h, h * h)
            found = [jnp.sum(term, axis=0, keepdims=True) for term in terms]
            sums = found if sums is None else [a + r for a, r in zip(sums, found)]
    sums = [row[:, :half] + row[:, half:] for row in sums] + [jnp.zeros((1, half), f32)]
    rows = [jnp.concatenate(sums[i : i + 2], axis=1) for i in range(0, len(sums), 2)]
    rest = jnp.zeros((gram_ref.shape[1] - len(rows), 2 * half), f32)
    gram_ref[...] = jnp.broadcast_to(jnp.concatenate(rows + [rest], axis=0)[None], gram_ref.shape)


def times(a, b):
    return (a[0] * b[0] - a[1] * b[1], a[0] * b[1] + a[1] * b[0])


def conj_times(a, b):
    return (a[0] * b[0] + a[1] * b[1], a[0] * b[1] - a[1] * b[0])


def plus(*terms):
    return (sum(t[0] for t in terms), sum(t[1] for t in terms))


def scaled(a, r):
    return (a[0] * r, a[1] * r)


def finish_body(
    entries, gram_ref, x_ref, g_ref, g_other_ref, h_ref, h_other_ref, basis_ref, residual_ref, hess_ref
):
    devices = gram_ref.shape[0]
    parts = [gram_ref[i] for i in range(2)]
    for i in range(2, devices):
        parts[i % 2] = parts[i % 2] + gram_ref[i]
    low, high = (part / entries for part in parts)
    half = low.shape[1] // 2
    row = []
    for i in range(9):
        at = (slice(i // 2, i // 2 + 1), slice(i % 2 * half, (i % 2 + 1) * half))
        row.append(jnp.concatenate([low[at], high[at]], axis=1))
    xx, gg, hh = row[0], row[3], row[8]
    xg, xh, gh = (row[1], row[2]), (row[4], row[5]), (row[6], row[7])
    square = xx + epsilon
    beta = jnp.sqrt(square)
    inv = 1.0 / beta
    h11 = ((xx - xg[0]) / square, -xg[1] / square)
    alpha = ((epsilon + xg[0]) / square * inv, xg[1] / square * inv)
    delta = -inv
    cross = alpha[0] * xg[0] + alpha[1] * xg[1]
    norm = (alpha[0] * alpha[0] + alpha[1] * alpha[1]) * xx + delta * delta * gg + 2.0 * delta * cross
    h21 = jnp.sqrt(jnp.maximum(norm, 0.0) + epsilon)
    a = (alpha[0] / h21, alpha[1] / h21)
    d = delta / h21
    b = (d - a[0], -a[1])
    h12 = scaled(plus(scaled(a, xx), times(b, xg), scaled(xh, -d)), inv)
    e = (a[0] - h12[0] * inv, a[1] - h12[1] * inv)
    with_x = plus(scaled(e, xx), times(b, xg), scaled(xh, -d))
    with_g = plus(times(e, (xg[0], -xg[1])), scaled(b, gg), scaled(gh, -d))
    h22 = plus(conj_times(a, with_x), scaled(with_g, d))
    c0 = plus(e, scaled(times(h22, a), -1.0))
    c1 = plus(b, scaled(h22, -d))
    c2 = -d
    last = (
        (c0[0] * c0[0] + c0[1] * c0[1]) * xx
        + (c1[0] * c1[0] + c1[1] * c1[1]) * gg
        + c2 * c2 * hh
        + 2.0 * times(conj_times(c0, c1), xg)[0]
        + 2.0 * c2 * conj_times(c0, xh)[0]
        + 2.0 * c2 * conj_times(c1, gh)[0]
    )
    h32 = jnp.sqrt(jnp.maximum(last, 0.0) + epsilon)
    for i, value in enumerate((beta, h11[0], h11[1], h21, h12[0], h12[1], h22[0], h22[1], h32)):
        hess_ref[i : i + 1, :] = value
    count = g_ref.shape[1]

    def whole(mine, other):
        low, high = jnp.where(second(), other, mine), jnp.where(second(), mine, other)
        return tuple(
            jnp.concatenate([low[:, at : at + half], high[:, at : at + half]], axis=1) for at in (0, half)
        )

    for s in range(g_ref.shape[0]):
        rows = [pl.ds(z, count, stride=2) for z in range(2)]
        x = (x_ref[s, rows[0], :], x_ref[s, rows[1], :])
        g = whole(g_ref[s], g_other_ref[s])
        h = whole(h_ref[s], h_other_ref[s])
        basis = plus(times(a, x), scaled(g, d))
        residual = plus(times(c0, x), times(c1, g), scaled(h, c2))
        for z in range(2):
            basis_ref[s, rows[z], :] = basis[z]
            residual_ref[s, rows[z], :] = residual[z]


def trade(value, axis, bit):
    return lax.ppermute(value, axis, [(i, i ^ bit) for i in range(lax.axis_size(axis))])


def trade_odd(value):
    count = lax.axis_size("slab")
    pairs = []
    for i in range(count):
        pairs.append((i, (i + 1) % count if i % 2 else (i - 1) % count))
    return lax.ppermute(value, "slab", pairs)


def bits(axis, start=1):
    out, bit = [], start
    while bit < lax.axis_size(axis):
        out.append(bit)
        bit *= 2
    return out


def fetch_pieces(own):
    out = []
    even = trade(own, "slab", 1)
    groups = [jnp.stack([own, even]), trade_odd(own)]
    for group in groups:
        pieces = {0: group}
        for bit in bits("blk", 2):
            pieces.update({r | bit // 2: trade(value, "blk", bit) for r, value in list(pieces.items())})
        out += [pieces[r] for r in range(len(pieces))]
    return out


def total_sums(send, keep):
    steps = [("blk", bit) for bit in bits("blk", 2)] + [("slab", bit) for bit in bits("slab")]
    steps[1:3] = steps[2:0:-1]
    for axis, bit in steps:
        keep = keep + trade(send, axis, bit).astype(f32)
        send = keep.astype(bf16)
    return keep


def per_device(
    incident, mie_coef, translation, pair_shift, pair_member, positions, wave_index, plane_coef,
    ewald_weight,
):
    spheres, _, count, n = incident.shape
    pairs = translation.shape[1]
    blocks = lax.axis_size("blk")
    devices = blocks * lax.axis_size("slab")
    waves = plane_coef.shape[0]
    entries = spheres * lax.axis_size("slab") * count * blocks
    x = incident.transpose(0, 2, 1, 3).reshape(spheres, 2 * count, n)

    field = shape((spheres, count, n))
    both = shape((2, spheres, count, n))
    pair_half = shape((spheres, 2 * count, n), bf16)
    sums = shape((waves, n))
    sums_half = shape((waves, n), bf16)
    sources = shape((spheres, pairs, count * blocks, n), bf16)
    held_rows = -(-8 * spheres // 8) * 8
    column = shape((waves, held_rows))
    part = shape((2, 2, count, waves), bf16)

    def both_fields(own, send, keep):
        total = total_sums(send, keep)
        pieces = fetch_pieces(own)
        table = pltpu.SMEM((spheres, pairs), jnp.int32)
        buffers = [pltpu.VMEM((3 * spheres, count * blocks, n), bf16), table, table]
        buffers.append(pltpu.SemaphoreType.DMA((2,)))
        gathered = call(gather_body, sources, [HB, HB] + [VM] * blocks, buffers)(
            *in_hbm((pair_shift, pair_member)), *pieces
        )
        products = [
            jnp.einsum("ikarc,ikcn->ikarn", rows, gathered, preferred_element_type=f32)
            for rows in (rows_mine, rows_other)
        ]
        near = call(near_sum_body, both, [VM] * 2)(*products)
        return near, total

    mie_other = trade(mie_coef, "blk", 1)
    buffers = [pltpu.VMEM(x.shape, f32), pltpu.SemaphoreType.DMA]
    send, x_mine = call(split_body, (field, field), [HB], buffers)(*in_hbm([x]))
    x_other = trade(send, "blk", 1)
    stored = Layout(major_to_minor=(0, 1, 3, 2, 4))
    rows_mine = with_layout_constraint(translation, stored)
    operands = (
        plane_coef.transpose(1, 2, 0), wave_index.T, positions, ewald_weight.reshape(1, waves), mie_coef
    )
    buffers = [pltpu.VMEM(v.shape, v.dtype) for v in operands]
    buffers += [pltpu.VMEM((held_rows, waves), f32), pltpu.SemaphoreType.DMA((len(operands),))]
    columns, plane = call(
        tables_body, (column, part), [VM] + [HB] * len(operands), buffers
    )(mie_other, *in_hbm(operands))
    rounded, send, keep = call(first_sums_body, (pair_half, sums_half, sums), [VM] * 4)(x_mine, x_other, columns, plane)
    rows_other = with_layout_constraint(trade(rows_mine, "blk", 1), stored)
    near, total = both_fields(rounded, send, keep)
    tables = (shape((4 * spheres, waves, n)), shape((4 * spheres, count, n)))
    wide = call(spread_body, tables, [VM])(columns)
    g_mine, g_other, rounded, send, keep = call(
        first_image_body, (field, field, pair_half, sums_half, sums), [VM] * 5
    )(near, total, *wide, plane)
    g_back = trade(g_other, "blk", 1)
    near, total = both_fields(rounded, send, keep)
    h_mine, h_other, gram = call(
        second_image_body, (field, field, shape((devices, 8, n))), [VM] * 9
    )(near, total, *wide, plane, x_mine, x_other, g_mine, g_other)
    h_back = trade(h_other, "blk", 1)
    gram = lax.all_to_all(gram, ("slab", "blk"), 0, 0, tiled=True)
    flat = shape((spheres, 2 * count, n))
    basis, residual, hessenberg = call(
        lambda *refs: finish_body(float(entries), *refs), (flat, flat, shape((9, n))), [VM] * 6
    )(gram, x, g_mine, g_back, h_mine, h_back)

    def unflatten(value):
        return value.reshape(spheres, count, 2, n).transpose(0, 2, 1, 3)

    return unflatten(basis), unflatten(residual), hessenberg


def solution(mesh):
    placed = (
        P("slab", None, "blk", None),
        P("slab", None, "blk"),
        P("slab", None, None, "blk", None),
        P("slab", None),
        P("slab", None),
        P("slab", None),
        P(),
        P(),
        P(),
    )
    return jax.shard_map(
        per_device,
        mesh=mesh,
        in_specs=placed,
        out_specs=(P("slab", None, "blk", None), P("slab", None, "blk", None), P()),
        check_vma=False,
    )
```
